32 devices in a mesh: row: 8 (over y, x, core), col: 4 (over z).
Axes of the slice: x: 2, y: 2, z: 4, core: 2. Of those that a mesh axis runs over, the one named last changes fastest.
Arguments:
- residual: bfloat16 [8, 4, 2048, 512], P('row', 'col'), may hold values from -6 to 6
- self_tiles: bfloat16 [8, 4, 2048, 2048], P('row', 'col'), may hold values from -0.09375 to 0.09375
- side_tiles: bfloat16 [8, 4, 2048, 2048], P('row', 'col'), may hold values from -0.09375 to 0.09375
- row_cluster_basis: bfloat16 [8, 4, 2048, 32], P('row', 'col'), may hold values from -0.125 to 0.125
- column_cluster_basis: bfloat16 [8, 4, 2048, 32], P('row', 'col'), may hold values from -1 to 1
- couplings: bfloat16 [8, 4, 64, 32, 32], P('row', 'col'), may hold values from -0.1875 to 0.1875
- near_side: int32 [8, 4], P('row', 'col'), may hold values from -1 to 1
- adm_targets: int32 [8, 4, 64], P('row', 'col'), may hold values from 0 to 31, as said below
- adm_ranks: int32 [8, 4, 64], P('row', 'col'), may hold values from 8 to 32
- adm_count: int32 [8, 4], P('row', 'col'), may hold values from 1 to 64
Outputs:
- gradient: float32 [8, 4, 2048, 512], P('row', 'col')
The draws below stay inside these ranges and needn't reach their ends.
Inputs may be any that keep to these rules, and one draw needn't show every extreme that they name: `near_side`: -1 or +1 names the cluster row before or after around the loop of 8 rows; 0 means no such tile. Each entry of adm_targets for the block row of linear index i is the linear index of a cluster other than i; slot 0 names i - 1 or i + 1, counted round the 32 clusters; targets may repeat.
All inputs are finite; a program needn't handle non-finite values.
Results may differ from the reference program's by a relative error of at most 0.0033.
Values may be sent and summed in bfloat16 or wider, within the bound.
No kernel may reach another device: no remote copies, remote signals or barrier semaphores. Data moves between devices by JAX's collectives and lax.ppermute only.
A program may use at most 128 MiB of HBM per device.

```python
import jax
import jax.numpy as jnp
from jax import lax

LEAF = 2048
K = 32
NRHS = 512
ADM = 64
GRID_R = 8
GRID_C = 4


def draw_adm_targets(key, part):
    base = jax.random.fold_in(key, 11)
    first_key, second_key = jax.random.split(base)
    total = GRID_R * GRID_C
    linear = (jnp.arange(GRID_R, dtype=jnp.int32)[:, None] * GRID_C + jnp.arange(GRID_C, dtype=jnp.int32)[None, :])[:, :, None]
    offsets = jax.random.randint(first_key, (GRID_R, GRID_C, ADM), 1, total, dtype=jnp.int32)
    signs = jax.random.randint(second_key, (GRID_R, GRID_C, 1), 0, 2, dtype=jnp.int32) * 2 - 1
    slot_index = jnp.arange(ADM, dtype=jnp.int32)[None, None, :]
    chosen = jnp.where(slot_index == 0, signs + total, offsets)
    return ((linear + chosen) % total).astype(jnp.int32)


def plant(values, key, least, largest):
    shape = values.shape
    index_at = [jax.random.randint(jax.random.fold_in(key, axis), (), 0, shape[axis]) for axis in range(len(shape))]
    values = values.at[tuple(index_at)].set(least)
    longest = shape.index(max(shape))
    index_at[longest] = (index_at[longest] + 1) % shape[longest]
    return values.at[tuple(index_at)].set(largest)


def levels(stream_key, shape, cuts, least, high):
    factor_of = 1.0
    for dim, blocks in cuts:
        heights = jax.random.uniform(jax.random.fold_in(jax.random.fold_in(stream_key, 6), dim), (blocks,), jnp.float32, least / len(cuts), high / len(cuts))
        factor_of = factor_of * jnp.repeat(jnp.exp(heights), shape[dim] // blocks).reshape((-1,) + (1,) * (len(shape) - 1 - dim))
    return factor_of


def centred(stream_key, shape, width, limit, pieces=(), held_as=jnp.bfloat16):
    level = levels(stream_key, shape, pieces, -0.22, 0.18) if pieces else 1.0
    values = jax.random.normal(stream_key, shape, jnp.float32) * width * level
    return jnp.minimum(jnp.maximum(values, -limit), limit).astype(held_as)


def setup_inputs(seed: int = 0) -> dict:
    key_of = jax.random.split(jax.random.key(seed), 11)
    return {
        "residual": centred(key_of[0], (GRID_R, GRID_C, LEAF, NRHS), 1.0, 6.0, ((0, 8), (1, 4))),
        "self_tiles": centred(key_of[1], (GRID_R, GRID_C, LEAF, LEAF), (2 * LEAF) ** -0.5, 0.09375, ((0, 8), (1, 4))),
        "side_tiles": centred(key_of[2], (GRID_R, GRID_C, LEAF, LEAF), (2 * LEAF) ** -0.5, 0.09375, ((0, 8), (1, 4))),
        "row_cluster_basis": centred(key_of[3], (GRID_R, GRID_C, LEAF, K), LEAF ** -0.5, 0.125, ((0, 8), (1, 4))),
        "column_cluster_basis": centred(key_of[4], (GRID_R, GRID_C, LEAF, K), K ** -0.5, 1.0, ((0, 8), (1, 4))),
        "couplings": centred(key_of[5], (GRID_R, GRID_C, ADM, K, K), (K * ADM // 2) ** -0.5, 0.1875, ((0, 8), (1, 4))),
        "near_side": plant(jax.random.randint(key_of[6], (GRID_R, GRID_C), -1, 2), jax.random.fold_in(key_of[6], 1), -1, 1).astype(jnp.int32),
        "adm_targets": draw_adm_targets(jax.random.fold_in(key_of[10], 71), 0),
        "adm_ranks": plant(jax.random.randint(key_of[8], (GRID_R, GRID_C, ADM), K // 4, K + 1), jax.random.fold_in(key_of[8], 1), K // 4, K).astype(jnp.int32),
        "adm_count": plant(jax.random.randint(key_of[9], (GRID_R, GRID_C), 1, ADM + 1), jax.random.fold_in(key_of[9], 1), 1, ADM).astype(jnp.int32),
    }


def reference(residual, self_tiles, side_tiles, row_cluster_basis, column_cluster_basis, couplings, near_side, adm_targets, adm_ranks, adm_count):
    grid_rows, grid_cols, sample_points, columns = residual.shape
    slot_count = couplings.shape[2]
    rank_dimension = couplings.shape[3]
    cluster_groups = grid_rows * grid_cols
    flattened_result = residual.reshape(cluster_groups, sample_points, columns)
    coefficient_table = jnp.einsum("qhs,qhe->qse", row_cluster_basis.reshape(cluster_groups, sample_points, rank_dimension).astype(jnp.float32), flattened_result.astype(jnp.float32), precision=lax.Precision.HIGHEST).astype(jnp.bfloat16)
    rank_index = jnp.arange(rank_dimension, dtype=jnp.int32)
    slot_index = jnp.arange(slot_count, dtype=jnp.int32)
    keep_mask = (rank_index[None, None, None, :] < adm_ranks[:, :, :, None]) & (slot_index[None, None, :, None] < adm_count[:, :, None, None])
    keep_float = keep_mask.astype(jnp.float32)
    masked = couplings.astype(jnp.float32) * keep_float[:, :, :, :, None] * keep_float[:, :, :, None, :]
    masked = masked.reshape(cluster_groups, slot_count, rank_dimension, rank_dimension)
    targets = adm_targets.reshape(cluster_groups, slot_count).astype(jnp.int32)

    def add_row(running, inputs):
        block, coeff_block, target_row = inputs
        contrib = jnp.einsum("sab,an->sbn", block, coeff_block.astype(jnp.float32), precision=lax.Precision.HIGHEST)
        return running.at[target_row].add(contrib), jnp.zeros((), jnp.float32)

    result = lax.scan(add_row, jnp.zeros((cluster_groups, rank_dimension, columns), jnp.float32), (masked, coefficient_table, targets))
    dual_vector = result[0].astype(jnp.bfloat16)
    distant_part = jnp.einsum("qpo,qou->qpu", column_cluster_basis.reshape(cluster_groups, sample_points, rank_dimension).astype(jnp.float32), dual_vector.astype(jnp.float32), precision=lax.Precision.HIGHEST)
    from_above = jnp.roll(residual, 1, axis=0)
    from_below = jnp.roll(residual, -1, axis=0)
    side_offset = near_side[:, :, None, None]
    neighbour = jnp.where(side_offset == -1, from_above, jnp.where(side_offset == 1, from_below, jnp.zeros_like(residual)))

    def near_block(inputs):
        own_tile, own_res, side_tile, side_res = inputs
        own_part = jnp.dot(own_tile.T, own_res, preferred_element_type=jnp.float32)
        side_part = jnp.dot(side_tile.T, side_res, preferred_element_type=jnp.float32)
        return own_part + side_part

    near_part = lax.map(near_block, (self_tiles.reshape(cluster_groups, sample_points, sample_points), flattened_result, side_tiles.reshape(cluster_groups, sample_points, sample_points), neighbour.reshape(cluster_groups, sample_points, columns)))
    gradient = (near_part + distant_part).reshape(grid_rows, grid_cols, sample_points, columns)
    return gradient
```

```python
import jax
import jax.numpy as jnp
from jax import lax
from jax.sharding import PartitionSpec as P

CHUNKS = 8


def contract(tile, values):
    return lax.dot_general(
        tile, values, (((0,), (0,)), ((), ())), preferred_element_type=jnp.float32
    )


def dual_of(coefficients, couplings, targets, ranks, count):
    rows, cols = lax.axis_size("row"), lax.axis_size("col")
    slots, rank, _ = couplings.shape
    rank_index = jnp.arange(rank, dtype=jnp.int32)
    slot_index = jnp.arange(slots, dtype=jnp.int32)
    keep = (rank_index[None, :] < ranks[:, None]) & (slot_index < count)[:, None]
    keep = keep.astype(jnp.bfloat16)
    masked = couplings * keep[:, :, None] * keep[:, None, :]
    onehot = (targets[:, None] == jnp.arange(rows * cols, dtype=jnp.int32)[None, :]).astype(
        jnp.bfloat16
    )
    blocks = contract(onehot, masked.reshape(slots, rank * rank)).astype(jnp.bfloat16)
    blocks = blocks.reshape(rows, cols, rank, rank).transpose(1, 2, 0, 3)
    blocks = blocks.reshape(cols, rank, rows * rank)
    packed = jnp.concatenate(
        [jnp.broadcast_to(coefficients[None], (cols,) + coefficients.shape), blocks], axis=2
    )
    me = lax.axis_index("col")
    held = [lax.dynamic_index_in_dim(packed, me, 0, keepdims=False)]
    for shift in range(1, cols):
        outgoing = lax.dynamic_index_in_dim(packed, (me + shift) % cols, 0, keepdims=False)
        held.append(
            lax.ppermute(outgoing, "col", [(i, (i + shift) % cols) for i in range(cols)])
        )
    held = jnp.concatenate(held, axis=0)
    width = coefficients.shape[1]
    partial = contract(held[:, width:], held[:, :width])
    bits = rows.bit_length() - 1
    current = partial.reshape((2,) * bits + (rank, width))
    mine = lax.axis_index("row")
    left = list(range(bits))[::-1]
    for bit in [0] + list(range(bits - 1, 0, -1)):
        axis = left.index(bit)
        left.remove(bit)
        low = lax.index_in_dim(current, 0, axis, keepdims=False)
        high = lax.index_in_dim(current, 1, axis, keepdims=False)
        upper = (mine >> bit) & 1 == 1
        outgoing = jnp.where(upper, low, high).astype(jnp.bfloat16)
        kept = jnp.where(upper, high, low)
        incoming = lax.ppermute(outgoing, "row", [(i, i ^ (1 << bit)) for i in range(rows)])
        current = kept + incoming.astype(jnp.float32)
    return current.astype(jnp.bfloat16)


def on_device(
    residual,
    self_tiles,
    side_tiles,
    row_cluster_basis,
    column_cluster_basis,
    couplings,
    near_side,
    adm_targets,
    adm_ranks,
    adm_count,
):
    rows = lax.axis_size("row")
    local = residual[0, 0]
    points = local.shape[0]
    size = points // CHUNKS
    near_pairs = [(i, i ^ 1) for i in range(rows)]
    far_pairs = [(i, (i - 1) % rows if i % 2 == 0 else (i + 1) % rows) for i in range(rows)]
    side_offset = near_side[0, 0]
    near_offset = 1 - 2 * (lax.axis_index("row") % 2)
    use_near = side_offset == near_offset
    use_far = side_offset == -near_offset

    far = []
    for c in range(CHUNKS):
        piece = lax.slice_in_dim(local, c * size, (c + 1) * size)
        far.append(lax.ppermute(piece, "row", far_pairs))
    near = lax.ppermute(local, "row", near_pairs)
    coefficients = contract(row_cluster_basis[0, 0], local).astype(jnp.bfloat16)
    dual = dual_of(
        coefficients, couplings[0, 0], adm_targets[0, 0], adm_ranks[0, 0], adm_count[0, 0]
    )
    total = contract(self_tiles[0, 0], local)
    zero = jnp.zeros((), jnp.bfloat16)
    for c in range(CHUNKS):
        here = lax.slice_in_dim(near, c * size, (c + 1) * size)
        values = jnp.where(use_far, far[c], jnp.where(use_near, here, zero))
        tile = lax.slice_in_dim(side_tiles[0, 0], c * size, (c + 1) * size)
        total = lax.optimization_barrier(total)
        total = total + contract(tile, values)
        if c == CHUNKS - 2:
            total = lax.optimization_barrier(total)
            total = total + jnp.dot(
                column_cluster_basis[0, 0], dual, preferred_element_type=jnp.float32
            )
    return total[None, None]


def solution(mesh):
    placed = (
        P("row", "col", None, None),
        P("row", "col", None, None),
        P("row", "col", None, None),
        P("row", "col", None, None),
        P("row", "col", None, None),
        P("row", "col", None, None, None),
        P("row", "col"),
        P("row", "col", None),
        P("row", "col", None),
        P("row", "col"),
    )

    return jax.shard_map(
        on_device,
        mesh=mesh,
        in_specs=placed,
        out_specs=P("row", "col", None, None),
        check_vma=False,
    )
```

```python
import jax
import jax.numpy as jnp
from jax import lax
from jax.experimental import pallas as pl
from jax.experimental.pallas import tpu as pltpu
from jax.sharding import PartitionSpec as P

BLOCK = 512
GRANT = 20 * 1024 * 1024


def contract(tile, values):
    return lax.dot_general(
        tile, values, (((0,), (0,)), ((), ())), preferred_element_type=jnp.float32
    )


def in_vmem(value):
    return pltpu.with_memory_space_constraint(value, pltpu.VMEM)


def in_hbm(value):
    return pltpu.with_memory_space_constraint(value, pltpu.HBM)


def whole():
    return pl.BlockSpec(memory_space=pltpu.VMEM)


def grant():
    return pltpu.CompilerParams(vmem_limit_bytes=GRANT)


def split_rows(values, bounds, keep):
    columns = values.shape[1]

    def kernel(values_ref, *rest):
        outs, held, sems = rest[: len(bounds)], rest[len(bounds) : -1], rest[-1]
        held = outs if keep else held
        reads = [
            pltpu.make_async_copy(values_ref.at[pl.ds(start, size)], ref, sems.at[c])
            for c, ((start, size), ref) in enumerate(zip(bounds, held))
        ]
        for read in reads:
            read.start()
        writes = []
        for c, read in enumerate(reads):
            read.wait()
            if not keep:
                write = pltpu.make_async_copy(held[c], outs[c], sems.at[c + len(bounds)])
                write.start()
                writes.append(write)
        for write in writes:
            write.wait()

    shapes = [(size, columns) for _, size in bounds]
    space = pltpu.VMEM if keep else pltpu.HBM
    scratch = [] if keep else [pltpu.VMEM(shape, values.dtype) for shape in shapes]
    return pl.pallas_call(
        kernel,
        in_specs=[pl.BlockSpec(memory_space=pltpu.HBM)],
        out_specs=[pl.BlockSpec(memory_space=space) for _ in bounds],
        out_shape=[space(shape, values.dtype) for shape in shapes],
        scratch_shapes=scratch + [pltpu.SemaphoreType.DMA((2 * len(bounds),))],
        compiler_params=grant(),
    )(in_hbm(values))


def own_product(tile, values, part, parts, total=None):
    points, columns = tile.shape[1], values.shape[1]
    block = min(BLOCK, points // parts)
    steps = points // parts // block
    first = part * steps

    def kernel(tile_ref, values_ref, *rest):
        rest[-1][...] = contract(tile_ref[...], values_ref[...])

    in_specs = [
        pl.BlockSpec((tile.shape[0], block), lambda i: (0, first + i)),
        whole(),
    ]
    arguments = [in_hbm(tile), in_vmem(values)]
    if total is not None:
        in_specs.append(pl.BlockSpec(memory_space=pltpu.HBM))
        arguments.append(in_hbm(total))
    return pl.pallas_call(
        kernel,
        grid=(steps,),
        in_specs=in_specs,
        out_specs=pl.BlockSpec((block, columns), lambda i: (first + i, 0)),
        out_shape=pltpu.HBM((points, columns), jnp.float32),
        input_output_aliases={} if total is None else {2: 0},
        compiler_params=grant(),
        cost_estimate=pl.CostEstimate(
            flops=2 * tile.size * columns // parts,
            bytes_accessed=4 * tile.size // parts,
            transcendentals=0,
        ),
    )(*arguments)


def step_rows(block):
    return pl.ds(pl.multiple_of(pl.program_id(0) * block, block), block)


def choose(which_ref, far_refs, near_ref, values_ref):
    @pl.when(which_ref[0] == 2)
    def _():
        row = 0
        for far_ref in far_refs:
            values_ref[row : row + far_ref.shape[0], :] = far_ref[...]
            row += far_ref.shape[0]

    @pl.when(which_ref[0] == 1)
    def _():
        values_ref[...] = near_ref[...]

    @pl.when(which_ref[0] == 0)
    def _():
        values_ref[...] = jnp.zeros_like(values_ref)


def prepare_last(tile, near, start, size):
    points, columns = tile.shape[1], near.shape[1]
    block = min(BLOCK, points)
    at = start // size

    def kernel(tile_ref, near_ref, flipped_ref, kept_ref):
        flipped_ref[step_rows(block), :] = tile_ref[...].T

        @pl.when(pl.program_id(0) == 0)
        def _():
            kept_ref[...] = near_ref[...]

    return pl.pallas_call(
        kernel,
        grid=(points // block,),
        in_specs=[
            pl.BlockSpec((size, block), lambda i: (at, i)),
            pl.BlockSpec((size, columns), lambda i: (at, 0)),
        ],
        out_specs=[whole(), whole()],
        out_shape=[
            pltpu.VMEM((points, size), tile.dtype),
            pltpu.VMEM((size, columns), near.dtype),
        ],
        compiler_params=grant(),
    )(in_hbm(tile), in_hbm(near))


def add_rows(total, tile, far, near, which, start, extra):
    points, columns = total.shape
    size = sum(piece.shape[0] for piece in far)
    block = min(BLOCK, points)
    at = start // size
    count = len(far)

    def kernel(which_ref, total_ref, tile_ref, near_ref, *rest):
        out_ref, values_ref = rest[-2:]
        basis_ref, kept_ref, incoming_ref = rest[count:-2]
        here = step_rows(block)

        @pl.when(pl.program_id(0) == 0)
        def _():
            choose(which_ref, rest[:count], near_ref, values_ref)

        dual = (kept_ref[...] + incoming_ref[...].astype(jnp.float32)).astype(jnp.bfloat16)
        result = total_ref[...] + contract(tile_ref[...], values_ref[...])
        out_ref[here, :] = result + contract(basis_ref[:, here], dual)

    in_specs = [
        pl.BlockSpec(memory_space=pltpu.SMEM),
        pl.BlockSpec((block, columns), lambda i: (i, 0)),
        pl.BlockSpec((size, block), lambda i: (at, i)),
        pl.BlockSpec((size, columns), lambda i: (at, 0)),
    ]
    in_specs += [pl.BlockSpec(piece.shape, lambda i: (0, 0)) for piece in far]
    in_specs += [whole() for _ in extra]
    return pl.pallas_call(
        kernel,
        grid=(points // block,),
        in_specs=in_specs,
        out_specs=whole(),
        out_shape=pltpu.VMEM((points, columns), jnp.float32),
        compiler_params=grant(),
        scratch_shapes=[pltpu.VMEM((size, columns), jnp.bfloat16)],
        cost_estimate=pl.CostEstimate(
            flops=2 * size * points * columns,
            bytes_accessed=2 * size * points + 8 * total.size,
            transcendentals=0,
        ),
    )(
        which,
        in_hbm(total),
        in_hbm(tile),
        in_hbm(near),
        *[in_hbm(piece) for piece in far],
        *[in_vmem(value) for value in extra],
    )


def add_last(total, flipped, far, near, which):
    points, columns = total.shape
    size = far.shape[0]
    block = min(BLOCK // 2, points)
    steps = points // block

    def kernel(which_ref, total_ref, flipped_ref, far_ref, near_ref, out_ref, *scratch):
        values_ref, staged_ref, sems = scratch
        choose(which_ref, [far_ref], near_ref, values_ref)
        copies = []
        for step in range(steps):
            rows = pl.ds(step * block, block)
            staged_ref[rows, :] = total_ref[rows, :] + jnp.dot(
                flipped_ref[rows, :], values_ref[...], preferred_element_type=jnp.float32
            )
            copy = pltpu.make_async_copy(staged_ref.at[rows], out_ref.at[rows], sems.at[step])
            copy.start()
            copies.append(copy)
        for copy in copies:
            copy.wait()

    return pl.pallas_call(
        kernel,
        in_specs=[pl.BlockSpec(memory_space=pltpu.SMEM)] + [whole() for _ in range(4)],
        out_specs=pl.BlockSpec(memory_space=pltpu.HBM),
        out_shape=jax.ShapeDtypeStruct((points, columns), jnp.float32),
        compiler_params=grant(),
        scratch_shapes=[
            pltpu.VMEM((size, columns), jnp.bfloat16),
            pltpu.VMEM((points, columns), jnp.float32),
            pltpu.SemaphoreType.DMA((steps,)),
        ],
        cost_estimate=pl.CostEstimate(
            flops=2 * size * points * columns,
            bytes_accessed=2 * size * points + 8 * total.size,
            transcendentals=0,
        ),
    )(which, in_vmem(total), in_vmem(flipped), in_vmem(far), in_vmem(near))


def coupling_blocks(couplings, targets, ranks, count, rows, cols):
    slots, rank, _ = couplings.shape
    rank_index = jnp.arange(rank, dtype=jnp.int32)
    slot_index = jnp.arange(slots, dtype=jnp.int32)
    keep = (rank_index[None, :] < ranks[:, None]) & (slot_index < count)[:, None]
    keep = keep.astype(jnp.bfloat16)
    masked = couplings * keep[:, :, None] * keep[:, None, :]
    onehot = (targets[:, None] == jnp.arange(rows * cols, dtype=jnp.int32)[None, :]).astype(
        jnp.bfloat16
    )
    blocks = contract(onehot, masked.reshape(slots, rank * rank)).astype(jnp.bfloat16)
    blocks = blocks.reshape(rows, cols, rank, rank).transpose(1, 2, 0, 3)
    return blocks.reshape(cols, rank, rows * rank)


def dual_of(coefficients, blocks, rows, cols):
    rank, width = coefficients.shape
    packed = jnp.concatenate(
        [jnp.broadcast_to(coefficients[None], (cols,) + coefficients.shape), blocks], axis=2
    )
    me = lax.axis_index("col")
    held = [lax.dynamic_index_in_dim(packed, me, 0, keepdims=False)]
    for shift in range(1, cols):
        outgoing = lax.dynamic_index_in_dim(packed, (me + shift) % cols, 0, keepdims=False)
        held.append(lax.ppermute(outgoing, "col", [(i, (i + shift) % cols) for i in range(cols)]))
    held = jnp.concatenate(held, axis=0)
    partial = contract(held[:, width:], held[:, :width])
    bits = rows.bit_length() - 1
    current = partial.reshape((2,) * bits + (rank, width))
    mine = lax.axis_index("row")
    left = list(range(bits))[::-1]
    order = [0] + list(range(bits - 1, 0, -1))
    for place, bit in enumerate(order):
        axis = left.index(bit)
        left.remove(bit)
        low = lax.index_in_dim(current, 0, axis, keepdims=False)
        high = lax.index_in_dim(current, 1, axis, keepdims=False)
        upper = (mine >> bit) & 1 == 1
        outgoing = jnp.where(upper, low, high).astype(jnp.bfloat16)
        kept = jnp.where(upper, high, low)
        incoming = lax.ppermute(outgoing, "row", [(i, i ^ (1 << bit)) for i in range(rows)])
        if place < bits - 1:
            current = kept + incoming.astype(jnp.float32)
    return kept, incoming


def on_device(
    residual,
    self_tiles,
    side_tiles,
    row_cluster_basis,
    column_cluster_basis,
    couplings,
    near_side,
    adm_targets,
    adm_ranks,
    adm_count,
):
    rows, cols = lax.axis_size("row"), lax.axis_size("col")
    local = residual[0, 0]
    points = local.shape[0]
    near_pairs = [(i, i ^ 1) for i in range(rows)]
    far_pairs = [(i, (i - 1) % rows if i % 2 == 0 else (i + 1) % rows) for i in range(rows)]
    side_offset = near_side[0, 0]
    near_offset = 1 - 2 * (lax.axis_index("row") % 2)
    which = jnp.where(
        side_offset == 0, 0, jnp.where(side_offset == near_offset, 1, 2)
    ).astype(jnp.int32).reshape(1)

    unit = points // 8
    bounds = [(0, unit), (unit, 5 * unit), (6 * unit, 2 * unit)]
    pieces = split_rows(local, bounds[:1], True)
    pieces += split_rows(local, bounds[1:], False)
    far = []
    for piece in pieces:
        far.append(lax.ppermute(piece, "row", far_pairs))
    near = lax.ppermute(local, "row", near_pairs)
    coefficients = contract(row_cluster_basis[0, 0], local).astype(jnp.bfloat16)
    blocks = coupling_blocks(
        couplings[0, 0], adm_targets[0, 0], adm_ranks[0, 0], adm_count[0, 0], rows, cols
    )
    kept, incoming = dual_of(coefficients, blocks, rows, cols)
    total = own_product(self_tiles[0, 0], local, 0, 2)
    total = own_product(self_tiles[0, 0], local, 1, 2, total)
    side = side_tiles[0, 0]
    flipped, near_last = prepare_last(side, near, *bounds[2])
    extra = (column_cluster_basis[0, 0].T, kept, incoming)
    total = add_rows(total, side, far[:2], near, which, bounds[0][0], extra)
    total = add_last(total, flipped, far[2], near_last, which)
    return total[None, None]


def solution(mesh):
    placed = (
        P("row", "col", None, None),
        P("row", "col", None, None),
        P("row", "col", None, None),
        P("row", "col", None, None),
        P("row", "col", None, None),
        P("row", "col", None, None, None),
        P("row", "col"),
        P("row", "col", None),
        P("row", "col", None),
        P("row", "col"),
    )

    return jax.shard_map(
        on_device,
        mesh=mesh,
        in_specs=placed,
        out_specs=P("row", "col", None, None),
        check_vma=False,
    )
```

```python
import jax
import jax.numpy as jnp
from jax import lax
from jax.experimental import pallas as pl
from jax.experimental.pallas import tpu as pltpu
from jax.sharding import PartitionSpec as P

BLOCK = 512
GRANT = 20 * 1024 * 1024


def contract(tile, values):
    return lax.dot_general(
        tile, values, (((0,), (0,)), ((), ())), preferred_element_type=jnp.float32
    )


def in_vmem(value):
    return pltpu.with_memory_space_constraint(value, pltpu.VMEM)


def in_hbm(value):
    return pltpu.with_memory_space_constraint(value, pltpu.HBM)


def whole():
    return pl.BlockSpec(memory_space=pltpu.VMEM)


def grant():
    return pltpu.CompilerParams(vmem_limit_bytes=GRANT)


def split(values, bounds):
    def kernel(values_ref, *rest):
        outs, held, sems = rest[: len(bounds)], rest[len(bounds) : -1], rest[-1]
        reads = [
            pltpu.make_async_copy(
                values_ref.at[pl.ds(row, size), pl.ds(column, width)], ref, sems.at[c]
            )
            for c, ((row, size, column, width), ref) in enumerate(zip(bounds, held))
        ]
        for read in reads:
            read.start()
        writes = []
        for c, read in enumerate(reads):
            read.wait()
            write = pltpu.make_async_copy(held[c], outs[c], sems.at[c + len(bounds)])
            write.start()
            writes.append(write)
        for write in writes:
            write.wait()

    shapes = [(size, width) for _, size, _, width in bounds]
    scratch = [pltpu.VMEM(shape, values.dtype) for shape in shapes]
    return pl.pallas_call(
        kernel,
        in_specs=[pl.BlockSpec(memory_space=pltpu.HBM)],
        out_specs=[pl.BlockSpec(memory_space=pltpu.HBM) for _ in bounds],
        out_shape=[pltpu.HBM(shape, values.dtype) for shape in shapes],
        scratch_shapes=scratch + [pltpu.SemaphoreType.DMA((2 * len(bounds),))],
        compiler_params=grant(),
    )(in_hbm(values))


def own_product(tile, values, part, parts, total=None):
    points, columns = tile.shape[1], values.shape[1]
    block = min(BLOCK, points // parts)
    steps = points // parts // block
    first = part * steps

    def kernel(tile_ref, values_ref, *rest):
        rest[-1][...] = contract(tile_ref[...], values_ref[...])

    in_specs = [
        pl.BlockSpec((tile.shape[0], block), lambda i: (0, first + i)),
        whole(),
    ]
    arguments = [in_hbm(tile), in_vmem(values)]
    if total is not None:
        in_specs.append(pl.BlockSpec(memory_space=pltpu.HBM))
        arguments.append(in_hbm(total))
    return pl.pallas_call(
        kernel,
        grid=(steps,),
        in_specs=in_specs,
        out_specs=pl.BlockSpec((block, columns), lambda i: (first + i, 0)),
        out_shape=pltpu.HBM((points, columns), jnp.float32),
        input_output_aliases={} if total is None else {2: 0},
        compiler_params=grant(),
        cost_estimate=pl.CostEstimate(
            flops=2 * tile.size * columns // parts,
            bytes_accessed=4 * tile.size // parts,
            transcendentals=0,
        ),
    )(*arguments)


def step_rows(block):
    return pl.ds(pl.multiple_of(pl.program_id(0) * block, block), block)


def choose(which_ref, far_refs, near_ref, values_ref):
    @pl.when(which_ref[0] == 2)
    def _():
        row = 0
        for far_ref in far_refs:
            values_ref[row : row + far_ref.shape[0], :] = far_ref[...]
            row += far_ref.shape[0]

    @pl.when(which_ref[0] == 1)
    def _():
        values_ref[...] = near_ref[...]

    @pl.when(which_ref[0] == 0)
    def _():
        values_ref[...] = jnp.zeros_like(values_ref)


def prepare_last(tile, near, start, size):
    points, columns = tile.shape[1], near.shape[1]
    block = min(BLOCK, points)
    at = start // size

    def kernel(tile_ref, near_ref, flipped_ref, kept_ref):
        flipped_ref[step_rows(block), :] = tile_ref[...].T

        @pl.when(pl.program_id(0) == 0)
        def _():
            kept_ref[...] = near_ref[...]

    return pl.pallas_call(
        kernel,
        grid=(points // block,),
        in_specs=[
            pl.BlockSpec((size, block), lambda i: (at, i)),
            pl.BlockSpec((size, columns), lambda i: (at, 0)),
        ],
        out_specs=[whole(), whole()],
        out_shape=[
            pltpu.VMEM((points, size), tile.dtype),
            pltpu.VMEM((size, columns), near.dtype),
        ],
        compiler_params=grant(),
    )(in_hbm(tile), in_hbm(near))


def add_rows(total, tile, far, near, which, start, extra):
    points, columns = total.shape
    size = sum(piece.shape[0] for piece in far)
    block = min(BLOCK, points)
    at = start // size
    count = len(far)

    def kernel(which_ref, total_ref, tile_ref, near_ref, *rest):
        out_ref, values_ref = rest[-2:]
        basis_ref, kept_ref, incoming_ref = rest[count:-2]
        here = step_rows(block)

        @pl.when(pl.program_id(0) == 0)
        def _():
            choose(which_ref, rest[:count], near_ref, values_ref)

        dual = (kept_ref[...] + incoming_ref[...].astype(jnp.float32)).astype(jnp.bfloat16)
        result = total_ref[...] + contract(tile_ref[...], values_ref[...])
        out_ref[here, :] = result + contract(basis_ref[:, here], dual)

    in_specs = [
        pl.BlockSpec(memory_space=pltpu.SMEM),
        pl.BlockSpec((block, columns), lambda i: (i, 0)),
        pl.BlockSpec((size, block), lambda i: (at, i)),
        pl.BlockSpec((size, columns), lambda i: (at, 0)),
    ]
    in_specs += [pl.BlockSpec(piece.shape, lambda i: (0, 0)) for piece in far]
    in_specs += [whole() for _ in extra]
    return pl.pallas_call(
        kernel,
        grid=(points // block,),
        in_specs=in_specs,
        out_specs=whole(),
        out_shape=pltpu.VMEM((points, columns), jnp.float32),
        compiler_params=grant(),
        scratch_shapes=[pltpu.VMEM((size, columns), jnp.bfloat16)],
        cost_estimate=pl.CostEstimate(
            flops=2 * size * points * columns,
            bytes_accessed=2 * size * points + 8 * total.size,
            transcendentals=0,
        ),
    )(
        which,
        in_hbm(total),
        in_hbm(tile),
        in_hbm(near),
        *[in_hbm(piece) for piece in far],
        *[in_vmem(value) for value in extra],
    )


def add_last(total, flipped, far, near, which, column, out=None):
    points, columns = total.shape
    size, width = far.shape
    block = min(BLOCK // 2, points)
    steps = points // block
    here = pl.ds(column, width)

    def kernel(which_ref, total_ref, flipped_ref, far_ref, near_ref, *rest):
        out_ref, values_ref, staged_ref, sems = rest[-4:]
        choose(which_ref, [far_ref], near_ref.at[:, here], values_ref)
        copies = []
        for step in range(steps):
            rows = pl.ds(step * block, block)
            staged_ref[rows, :] = total_ref[rows, here] + jnp.dot(
                flipped_ref[rows, :], values_ref[...], preferred_element_type=jnp.float32
            )
            copy = pltpu.make_async_copy(
                staged_ref.at[rows], out_ref.at[rows, here], sems.at[step]
            )
            copy.start()
            copies.append(copy)
        for copy in copies:
            copy.wait()

    arguments = [which] + [in_vmem(value) for value in (total, flipped, far, near)]
    in_specs = [pl.BlockSpec(memory_space=pltpu.SMEM)] + [whole() for _ in range(4)]
    if out is not None:
        arguments.append(in_hbm(out))
        in_specs.append(pl.BlockSpec(memory_space=pltpu.HBM))
    return pl.pallas_call(
        kernel,
        in_specs=in_specs,
        out_specs=pl.BlockSpec(memory_space=pltpu.HBM),
        out_shape=jax.ShapeDtypeStruct((points, columns), jnp.float32),
        input_output_aliases={} if out is None else {5: 0},
        compiler_params=grant(),
        scratch_shapes=[
            pltpu.VMEM((size, width), jnp.bfloat16),
            pltpu.VMEM((points, width), jnp.float32),
            pltpu.SemaphoreType.DMA((steps,)),
        ],
        cost_estimate=pl.CostEstimate(
            flops=2 * size * points * width,
            bytes_accessed=2 * size * points + 8 * points * width,
            transcendentals=0,
        ),
    )(*arguments)


def coupling_blocks(couplings, targets, ranks, count, rows, cols):
    slots, rank, _ = couplings.shape
    rank_index = jnp.arange(rank, dtype=jnp.int32)
    slot_index = jnp.arange(slots, dtype=jnp.int32)
    keep = (rank_index[None, :] < ranks[:, None]) & (slot_index < count)[:, None]
    keep = keep.astype(jnp.bfloat16)
    masked = couplings * keep[:, :, None] * keep[:, None, :]
    onehot = (targets[:, None] == jnp.arange(rows * cols, dtype=jnp.int32)[None, :]).astype(
        jnp.bfloat16
    )
    sums = contract(onehot, masked.reshape(slots, rank * rank))
    high = lax.reduce_precision(sums, 8, 7)
    parts = [high.astype(jnp.bfloat16), (sums - high).astype(jnp.bfloat16)]
    blocks = jnp.stack(parts).reshape(2, rows, cols, rank, rank).transpose(2, 3, 0, 1, 4)
    return blocks.reshape(cols, rank, 2 * rows * rank)


def dual_of(coefficients, blocks, rows, cols):
    rank, width = coefficients.shape
    packed = jnp.concatenate(
        [jnp.broadcast_to(coefficients[None], (cols,) + coefficients.shape), blocks], axis=2
    )
    me = lax.axis_index("col")
    held = [lax.dynamic_index_in_dim(packed, me, 0, keepdims=False)]
    for shift in range(1, cols):
        outgoing = lax.dynamic_index_in_dim(packed, (me + shift) % cols, 0, keepdims=False)
        held.append(lax.ppermute(outgoing, "col", [(i, (i + shift) % cols) for i in range(cols)]))
    held = jnp.concatenate(held, axis=0)
    half = width + rows * rank
    partial = contract(held[:, width:half], held[:, :width])
    partial = partial + contract(held[:, half:], held[:, :width])
    bits = rows.bit_length() - 1
    current = partial.reshape((2,) * bits + (rank, width))
    mine = lax.axis_index("row")
    left = list(range(bits))[::-1]
    order = [0] + list(range(bits - 1, 0, -1))
    for place, bit in enumerate(order):
        axis = left.index(bit)
        left.remove(bit)
        low = lax.index_in_dim(current, 0, axis, keepdims=False)
        high = lax.index_in_dim(current, 1, axis, keepdims=False)
        upper = (mine >> bit) & 1 == 1
        outgoing = jnp.where(upper, low, high)
        kept = jnp.where(upper, high, low)
        if place == bits - 1:
            outgoing = outgoing.astype(jnp.bfloat16)
        incoming = lax.ppermute(outgoing, "row", [(i, i ^ (1 << bit)) for i in range(rows)])
        if place < bits - 1:
            current = kept + incoming
    return kept, incoming


def on_device(
    residual,
    self_tiles,
    side_tiles,
    row_cluster_basis,
    column_cluster_basis,
    couplings,
    near_side,
    adm_targets,
    adm_ranks,
    adm_count,
):
    rows, cols = lax.axis_size("row"), lax.axis_size("col")
    local = residual[0, 0]
    points = local.shape[0]
    near_pairs = [(i, i ^ 1) for i in range(rows)]
    far_pairs = [(i, (i - 1) % rows if i % 2 == 0 else (i + 1) % rows) for i in range(rows)]
    side_offset = near_side[0, 0]
    near_offset = 1 - 2 * (lax.axis_index("row") % 2)
    which = jnp.where(
        side_offset == 0, 0, jnp.where(side_offset == near_offset, 1, 2)
    ).astype(jnp.int32).reshape(1)

    unit = points // 8
    width = local.shape[1]
    early = width * 3 // 4
    bounds = [
        (unit, 5 * unit, 0, width),
        (6 * unit, 2 * unit, 0, early),
        (6 * unit, 2 * unit, early, width - early),
    ]
    pieces = [lax.slice_in_dim(local, 0, unit), *split(local, bounds)]
    far = []
    for piece in pieces:
        far.append(lax.ppermute(piece, "row", far_pairs))
    near = lax.ppermute(local, "row", near_pairs)
    coefficients = contract(row_cluster_basis[0, 0], local).astype(jnp.bfloat16)
    blocks = coupling_blocks(
        couplings[0, 0], adm_targets[0, 0], adm_ranks[0, 0], adm_count[0, 0], rows, cols
    )
    kept, incoming = dual_of(coefficients, blocks, rows, cols)
    total = own_product(self_tiles[0, 0], local, 0, 2)
    total = own_product(self_tiles[0, 0], local, 1, 2, total)
    side = side_tiles[0, 0]
    flipped, near_last = prepare_last(side, near, 6 * unit, 2 * unit)
    extra = (column_cluster_basis[0, 0].T, kept, incoming)
    total = add_rows(total, side, far[:2], near, which, 0, extra)
    out = add_last(total, flipped, far[2], near_last, which, 0)
    out = add_last(total, flipped, far[3], near_last, which, early, out)
    return out[None, None]


def solution(mesh):
    placed = (
        P("row", "col", None, None),
        P("row", "col", None, None),
        P("row", "col", None, None),
        P("row", "col", None, None),
        P("row", "col", None, None),
        P("row", "col", None, None, None),
        P("row", "col"),
        P("row", "col", None),
        P("row", "col", None),
        P("row", "col"),
    )

    return jax.shard_map(
        on_device,
        mesh=mesh,
        in_specs=placed,
        out_specs=P("row", "col", None, None),
        check_vma=False,
    )
```

```python
import jax
import jax.numpy as jnp
from jax import lax
from jax.experimental import pallas as pl
from jax.experimental.pallas import tpu as pltpu
from jax.sharding import PartitionSpec as P

BLOCK = 512
GRANT = 20 * 1024 * 1024


def contract(tile, values):
    return lax.dot_general(
        tile, values, (((0,), (0,)), ((), ())), preferred_element_type=jnp.float32
    )


def in_vmem(value):
    return pltpu.with_memory_space_constraint(value, pltpu.VMEM)


def in_hbm(value):
    return pltpu.with_memory_space_constraint(value, pltpu.HBM)


def whole():
    return pl.BlockSpec(memory_space=pltpu.VMEM)


def grant():
    return pltpu.CompilerParams(vmem_limit_bytes=GRANT)


def split(values, bounds):
    def kernel(values_ref, *rest):
        outs, held, sems = rest[: len(bounds)], rest[len(bounds) : -1], rest[-1]
        reads = [
            pltpu.make_async_copy(
                values_ref.at[pl.ds(row, size), pl.ds(column, width)], ref, sems.at[c]
            )
            for c, ((row, size, column, width), ref) in enumerate(zip(bounds, held))
        ]
        for read in reads:
            read.start()
        writes = []
        for c, read in enumerate(reads):
            read.wait()
            write = pltpu.make_async_copy(held[c], outs[c], sems.at[c + len(bounds)])
            write.start()
            writes.append(write)
        for write in writes:
            write.wait()

    shapes = [(size, width) for _, size, _, width in bounds]
    scratch = [pltpu.VMEM(shape, values.dtype) for shape in shapes]
    return pl.pallas_call(
        kernel,
        in_specs=[pl.BlockSpec(memory_space=pltpu.HBM)],
        out_specs=[pl.BlockSpec(memory_space=pltpu.HBM) for _ in bounds],
        out_shape=[pltpu.HBM(shape, values.dtype) for shape in shapes],
        scratch_shapes=scratch + [pltpu.SemaphoreType.DMA((2 * len(bounds),))],
        compiler_params=grant(),
    )(in_hbm(values))


def own_product(tile, values, part, parts, total=None):
    points, columns = tile.shape[1], values.shape[1]
    block = min(BLOCK, points // parts)
    steps = points // parts // block
    first = part * steps

    def kernel(tile_ref, values_ref, *rest):
        rest[-1][...] = contract(tile_ref[...], values_ref[...])

    in_specs = [
        pl.BlockSpec((tile.shape[0], block), lambda i: (0, first + i)),
        whole(),
    ]
    arguments = [in_hbm(tile), in_vmem(values)]
    if total is not None:
        in_specs.append(pl.BlockSpec(memory_space=pltpu.HBM))
        arguments.append(in_hbm(total))
    return pl.pallas_call(
        kernel,
        grid=(steps,),
        in_specs=in_specs,
        out_specs=pl.BlockSpec((block, columns), lambda i: (first + i, 0)),
        out_shape=pltpu.HBM((points, columns), jnp.float32),
        input_output_aliases={} if total is None else {2: 0},
        compiler_params=grant(),
        cost_estimate=pl.CostEstimate(
            flops=2 * tile.size * columns // parts,
            bytes_accessed=4 * tile.size // parts,
            transcendentals=0,
        ),
    )(*arguments)


def step_rows(block):
    return pl.ds(pl.multiple_of(pl.program_id(0) * block, block), block)


def choose(which_ref, fetch, near_ref, values_ref):
    @pl.when(which_ref[0] == 2)
    def _():
        fetch()

    @pl.when(which_ref[0] == 1)
    def _():
        values_ref[...] = near_ref[...]

    @pl.when(which_ref[0] == 0)
    def _():
        values_ref[...] = jnp.zeros_like(values_ref)


def stage(tile, near, total, start):
    rows, points = tile.shape
    size = rows - start
    block = min(BLOCK, points)

    def kernel(tile_ref, near_ref, total_ref, first_ref, flipped_ref, near_out, total_out, *scratch):
        last_ref, sems = scratch
        copies = [
            pltpu.make_async_copy(tile_ref.at[pl.ds(start, size)], last_ref, sems.at[0]),
            pltpu.make_async_copy(tile_ref.at[pl.ds(0, start)], first_ref, sems.at[1]),
            pltpu.make_async_copy(total_ref, total_out, sems.at[2]),
            pltpu.make_async_copy(near_ref, near_out, sems.at[3]),
        ]
        for copy in copies:
            copy.start()
        copies[0].wait()
        for at in range(0, points, block):
            flipped_ref[at : at + block, :] = last_ref[:, at : at + block].T
        for copy in copies[1:]:
            copy.wait()

    return pl.pallas_call(
        kernel,
        in_specs=[pl.BlockSpec(memory_space=pltpu.HBM) for _ in range(3)],
        out_specs=[whole() for _ in range(4)],
        out_shape=[
            pltpu.VMEM((start, points), tile.dtype),
            pltpu.VMEM((points, size), tile.dtype),
            pltpu.VMEM(near.shape, near.dtype),
            pltpu.VMEM(total.shape, total.dtype),
        ],
        compiler_params=grant(),
        scratch_shapes=[
            pltpu.VMEM((size, points), tile.dtype),
            pltpu.SemaphoreType.DMA((4,)),
        ],
    )(in_hbm(tile), in_hbm(near), in_hbm(total))


def add_rows(total, tile, far, near, which, extra):
    points, columns = total.shape
    size = tile.shape[0]
    block = min(BLOCK, points)
    count = len(far)

    def kernel(which_ref, total_ref, tile_ref, near_ref, *rest):
        out_ref, values_ref, sems = rest[-3:]
        basis_ref, kept_ref, incoming_ref = rest[count:-3]
        here = step_rows(block)

        def fetch():
            row, copies = 0, []
            for c, far_ref in enumerate(rest[:count]):
                rows = pl.ds(row, far_ref.shape[0])
                copies.append(pltpu.make_async_copy(far_ref, values_ref.at[rows], sems.at[c]))
                copies[-1].start()
                row += far_ref.shape[0]
            for copy in copies:
                copy.wait()

        @pl.when(pl.program_id(0) == 0)
        def _():
            choose(which_ref, fetch, near_ref.at[:size], values_ref)

        dual = (kept_ref[...] + incoming_ref[...].astype(jnp.float32)).astype(jnp.bfloat16)
        result = total_ref[here, :] + contract(tile_ref[:, here], values_ref[...])
        out_ref[here, :] = result + contract(basis_ref[:, here], dual)

    arguments = [which] + [in_vmem(value) for value in (total, tile, near)]
    arguments += [in_hbm(piece) for piece in far] + [in_vmem(value) for value in extra]
    in_specs = [pl.BlockSpec(memory_space=pltpu.SMEM)] + [whole() for _ in range(3)]
    in_specs += [pl.BlockSpec(memory_space=pltpu.HBM) for _ in far] + [whole() for _ in extra]
    return pl.pallas_call(
        kernel,
        grid=(points // block,),
        in_specs=in_specs,
        out_specs=whole(),
        out_shape=pltpu.VMEM((points, columns), jnp.float32),
        input_output_aliases={1: 0},
        compiler_params=grant(),
        scratch_shapes=[
            pltpu.VMEM((size, columns), jnp.bfloat16),
            pltpu.SemaphoreType.DMA((count,)),
        ],
        cost_estimate=pl.CostEstimate(
            flops=2 * size * points * columns,
            bytes_accessed=2 * size * columns,
            transcendentals=0,
        ),
    )(*arguments)


def add_last(total, flipped, far, near, which, column, out=None):
    points, columns = total.shape
    size, width = far.shape
    block = min(BLOCK // 2, points)
    steps = points // block
    here = pl.ds(column, width)

    def kernel(which_ref, total_ref, flipped_ref, far_ref, near_ref, *rest):
        out_ref, values_ref, staged_ref, sems = rest[-4:]

        def fetch():
            values_ref[...] = far_ref[...]

        choose(which_ref, fetch, near_ref.at[points - size :, here], values_ref)
        copies = []
        for step in range(steps):
            rows = pl.ds(step * block, block)
            staged_ref[rows, :] = total_ref[rows, here] + jnp.dot(
                flipped_ref[rows, :], values_ref[...], preferred_element_type=jnp.float32
            )
            copy = pltpu.make_async_copy(
                staged_ref.at[rows], out_ref.at[rows, here], sems.at[step]
            )
            copy.start()
            copies.append(copy)
        for copy in copies:
            copy.wait()

    arguments = [which] + [in_vmem(value) for value in (total, flipped, far, near)]
    in_specs = [pl.BlockSpec(memory_space=pltpu.SMEM)] + [whole() for _ in range(4)]
    if out is not None:
        arguments.append(in_hbm(out))
        in_specs.append(pl.BlockSpec(memory_space=pltpu.HBM))
    return pl.pallas_call(
        kernel,
        in_specs=in_specs,
        out_specs=pl.BlockSpec(memory_space=pltpu.HBM),
        out_shape=jax.ShapeDtypeStruct((points, columns), jnp.float32),
        input_output_aliases={} if out is None else {5: 0},
        compiler_params=grant(),
        scratch_shapes=[
            pltpu.VMEM((size, width), jnp.bfloat16),
            pltpu.VMEM((points, width), jnp.float32),
            pltpu.SemaphoreType.DMA((steps,)),
        ],
        cost_estimate=pl.CostEstimate(
            flops=2 * size * points * width,
            bytes_accessed=2 * size * points + 8 * points * width,
            transcendentals=0,
        ),
    )(*arguments)


def coupling_blocks(couplings, targets, ranks, count, rows, cols):
    slots, rank, _ = couplings.shape
    rank_index = jnp.arange(rank, dtype=jnp.int32)
    slot_index = jnp.arange(slots, dtype=jnp.int32)
    keep = (rank_index[None, :] < ranks[:, None]) & (slot_index < count)[:, None]
    keep = keep.astype(jnp.bfloat16)
    masked = couplings * keep[:, :, None] * keep[:, None, :]
    onehot = (targets[:, None] == jnp.arange(rows * cols, dtype=jnp.int32)[None, :]).astype(
        jnp.bfloat16
    )
    sums = contract(onehot, masked.reshape(slots, rank * rank))
    high = lax.reduce_precision(sums, 8, 7)
    parts = [high.astype(jnp.bfloat16), (sums - high).astype(jnp.bfloat16)]
    blocks = jnp.stack(parts).reshape(2, rows, cols, rank, rank).transpose(2, 3, 0, 1, 4)
    return blocks.reshape(cols, rank, 2 * rows * rank)


def dual_of(coefficients, blocks, rows, cols):
    rank, width = coefficients.shape
    packed = jnp.concatenate(
        [jnp.broadcast_to(coefficients[None], (cols,) + coefficients.shape), blocks], axis=2
    )
    me = lax.axis_index("col")
    held = [lax.dynamic_index_in_dim(packed, me, 0, keepdims=False)]
    for shift in range(1, cols):
        outgoing = lax.dynamic_index_in_dim(packed, (me + shift) % cols, 0, keepdims=False)
        held.append(lax.ppermute(outgoing, "col", [(i, (i + shift) % cols) for i in range(cols)]))
    held = jnp.concatenate(held, axis=0)
    half = width + rows * rank
    partial = contract(held[:, width:half], held[:, :width])
    partial = partial + contract(held[:, half:], held[:, :width])
    bits = rows.bit_length() - 1
    current = partial.reshape((2,) * bits + (rank, width))
    mine = lax.axis_index("row")
    left = list(range(bits))[::-1]
    order = [0] + list(range(bits - 1, 0, -1))
    for place, bit in enumerate(order):
        axis = left.index(bit)
        left.remove(bit)
        low = lax.index_in_dim(current, 0, axis, keepdims=False)
        high = lax.index_in_dim(current, 1, axis, keepdims=False)
        upper = (mine >> bit) & 1 == 1
        outgoing = jnp.where(upper, low, high)
        kept = jnp.where(upper, high, low)
        if place == bits - 1:
            outgoing = outgoing.astype(jnp.bfloat16)
        incoming = lax.ppermute(outgoing, "row", [(i, i ^ (1 << bit)) for i in range(rows)])
        if place < bits - 1:
            current = kept + incoming
    return kept, incoming


def on_device(
    residual,
    self_tiles,
    side_tiles,
    row_cluster_basis,
    column_cluster_basis,
    couplings,
    near_side,
    adm_targets,
    adm_ranks,
    adm_count,
):
    rows, cols = lax.axis_size("row"), lax.axis_size("col")
    local = residual[0, 0]
    points = local.shape[0]
    near_pairs = [(i, i ^ 1) for i in range(rows)]
    far_pairs = [(i, (i - 1) % rows if i % 2 == 0 else (i + 1) % rows) for i in range(rows)]
    side_offset = near_side[0, 0]
    near_offset = 1 - 2 * (lax.axis_index("row") % 2)
    which = jnp.where(
        side_offset == 0, 0, jnp.where(side_offset == near_offset, 1, 2)
    ).astype(jnp.int32).reshape(1)

    unit = points // 8
    width = local.shape[1]
    early = width * 3 // 4
    bounds = [
        (unit, 5 * unit, 0, width),
        (6 * unit, 2 * unit, 0, early),
        (6 * unit, 2 * unit, early, width - early),
    ]
    pieces = [lax.slice_in_dim(local, 0, unit), *split(local, bounds)]
    far = []
    for piece in pieces:
        far.append(lax.ppermute(piece, "row", far_pairs))
    near = lax.ppermute(local, "row", near_pairs)
    coefficients = contract(row_cluster_basis[0, 0], local).astype(jnp.bfloat16)
    blocks = coupling_blocks(
        couplings[0, 0], adm_targets[0, 0], adm_ranks[0, 0], adm_count[0, 0], rows, cols
    )
    kept, incoming = dual_of(coefficients, blocks, rows, cols)
    total = own_product(self_tiles[0, 0], local, 0, 2)
    total = own_product(self_tiles[0, 0], local, 1, 2, total)
    side = side_tiles[0, 0]
    first, flipped, near, total = stage(side, near, total, 6 * unit)
    extra = (column_cluster_basis[0, 0].T, kept, incoming)
    total = add_rows(total, first, far[:2], near, which, extra)
    out = add_last(total, flipped, far[2], near, which, 0)
    out = add_last(total, flipped, far[3], near, which, early, out)
    return out[None, None]


def solution(mesh):
    placed = (
        P("row", "col", None, None),
        P("row", "col", None, None),
        P("row", "col", None, None),
        P("row", "col", None, None),
        P("row", "col", None, None),
        P("row", "col", None, None, None),
        P("row", "col"),
        P("row", "col", None),
        P("row", "col", None),
        P("row", "col"),
    )

    return jax.shard_map(
        on_device,
        mesh=mesh,
        in_specs=placed,
        out_specs=P("row", "col", None, None),
        check_vma=False,
    )
```

```python
import jax
import jax.numpy as jnp
from jax import lax
from jax.experimental import pallas as pl
from jax.experimental.pallas import tpu as pltpu
from jax.sharding import PartitionSpec as P

BLOCK = 512
GRANT = 20 * 1024 * 1024


def contract(tile, values):
    return lax.dot_general(
        tile, values, (((0,), (0,)), ((), ())), preferred_element_type=jnp.float32
    )


def in_vmem(value):
    return pltpu.with_memory_space_constraint(value, pltpu.VMEM)


def in_hbm(value):
    return pltpu.with_memory_space_constraint(value, pltpu.HBM)


def whole():
    return pl.BlockSpec(memory_space=pltpu.VMEM)


def grant():
    return pltpu.CompilerParams(vmem_limit_bytes=GRANT)


def split(values, bounds, basis=None):
    def kernel(values_ref, *rest):
        count, sems = len(bounds), rest[-1]
        outs = rest[:count] if basis is None else rest[1 : 1 + count]
        copies = [
            pltpu.make_async_copy(
                values_ref.at[pl.ds(row, size), pl.ds(column, width)], out, sems.at[c]
            )
            for c, ((row, size, column, width), out) in enumerate(zip(bounds, outs))
        ]
        if basis is not None:
            copies.append(pltpu.make_async_copy(values_ref, rest[-3], sems.at[count]))
            copies.append(pltpu.make_async_copy(rest[0], rest[-2], sems.at[count + 1]))
        for copy in copies:
            copy.start()
        for copy in copies:
            copy.wait()
        if basis is not None:
            sums_ref = rest[1 + count]
            sums_ref[...] = jnp.dot(
                rest[-2][...], rest[-3][...], preferred_element_type=jnp.float32
            ).astype(sums_ref.dtype)

    shapes = [(size, width) for _, size, _, width in bounds]
    arguments = [in_hbm(values)]
    scratch = []
    if basis is not None:
        arguments.append(in_hbm(basis))
        shapes.append((basis.shape[0], values.shape[1]))
        scratch = [pltpu.VMEM(value.shape, value.dtype) for value in (values, basis)]
    return pl.pallas_call(
        kernel,
        in_specs=[pl.BlockSpec(memory_space=pltpu.HBM) for _ in arguments],
        out_specs=[whole() for _ in shapes],
        out_shape=[pltpu.VMEM(shape, values.dtype) for shape in shapes],
        scratch_shapes=scratch + [pltpu.SemaphoreType.DMA((len(bounds) + 2,))],
        compiler_params=grant(),
    )(*arguments)


def own_product(tile, values, part, parts, total=None):
    points, columns = tile.shape[1], values.shape[1]
    block = min(BLOCK, points // parts)
    steps = points // parts // block
    first = part * steps

    def kernel(tile_ref, values_ref, *rest):
        rest[-1][...] = contract(tile_ref[...], values_ref[...])

    in_specs = [
        pl.BlockSpec((tile.shape[0], block), lambda i: (0, first + i)),
        pl.BlockSpec(values.shape, lambda i: (0, 0)),
    ]
    arguments = [in_hbm(tile), in_hbm(values)]
    if total is not None:
        in_specs.append(pl.BlockSpec(memory_space=pltpu.HBM))
        arguments.append(in_hbm(total))
    return pl.pallas_call(
        kernel,
        grid=(steps,),
        in_specs=in_specs,
        out_specs=pl.BlockSpec((block, columns), lambda i: (first + i, 0)),
        out_shape=pltpu.HBM((points, columns), jnp.float32),
        input_output_aliases={} if total is None else {2: 0},
        compiler_params=grant(),
        cost_estimate=pl.CostEstimate(
            flops=2 * tile.size * columns // parts,
            bytes_accessed=4 * tile.size // parts,
            transcendentals=0,
        ),
    )(*arguments)


def step_rows(block):
    return pl.ds(pl.multiple_of(pl.program_id(0) * block, block), block)


def choose(which_ref, fetch, near_ref, values_ref):
    @pl.when(which_ref[0] == 2)
    def _():
        fetch()

    @pl.when(which_ref[0] == 1)
    def _():
        values_ref[...] = near_ref[...]

    @pl.when(which_ref[0] == 0)
    def _():
        values_ref[...] = jnp.zeros_like(values_ref)


def stage(tile, near, total, start):
    rows, points = tile.shape
    size = rows - start
    block = min(BLOCK, points)

    def kernel(tile_ref, near_ref, total_ref, first_ref, flipped_ref, near_out, total_out, *scratch):
        last_ref, sems = scratch
        copies = [
            pltpu.make_async_copy(tile_ref.at[pl.ds(start, size)], last_ref, sems.at[0]),
            pltpu.make_async_copy(tile_ref.at[pl.ds(0, start)], first_ref, sems.at[1]),
            pltpu.make_async_copy(total_ref, total_out, sems.at[2]),
            pltpu.make_async_copy(near_ref, near_out, sems.at[3]),
        ]
        for copy in copies:
            copy.start()
        copies[0].wait()
        for at in range(0, points, block):
            flipped_ref[at : at + block, :] = last_ref[:, at : at + block].T
        for copy in copies[1:]:
            copy.wait()

    return pl.pallas_call(
        kernel,
        in_specs=[pl.BlockSpec(memory_space=pltpu.HBM) for _ in range(3)],
        out_specs=[whole() for _ in range(4)],
        out_shape=[
            pltpu.VMEM((start, points), tile.dtype),
            pltpu.VMEM((points, size), tile.dtype),
            pltpu.VMEM(near.shape, near.dtype),
            pltpu.VMEM(total.shape, total.dtype),
        ],
        compiler_params=grant(),
        scratch_shapes=[
            pltpu.VMEM((size, points), tile.dtype),
            pltpu.SemaphoreType.DMA((4,)),
        ],
    )(in_hbm(tile), in_hbm(near), in_hbm(total))


def add_rows(total, tile, far, near, which, extra):
    points, columns = total.shape
    size = tile.shape[0]
    block = min(BLOCK, points)
    count = len(far)

    def kernel(which_ref, total_ref, tile_ref, near_ref, *rest):
        out_ref, values_ref, sems = rest[-3:]
        basis_ref, kept_ref, incoming_ref = rest[count:-3]
        here = step_rows(block)

        def fetch():
            lead = rest[0].shape[0]
            row, copies = lead, []
            values_ref[0:lead, :] = rest[0][...]
            for c, far_ref in enumerate(rest[1:count]):
                rows = pl.ds(row, far_ref.shape[0])
                copies.append(pltpu.make_async_copy(far_ref, values_ref.at[rows], sems.at[c]))
                copies[-1].start()
                row += far_ref.shape[0]
            for copy in copies:
                copy.wait()

        @pl.when(pl.program_id(0) == 0)
        def _():
            choose(which_ref, fetch, near_ref.at[:size], values_ref)

        dual = (kept_ref[...] + incoming_ref[...].astype(jnp.float32)).astype(jnp.bfloat16)
        result = total_ref[here, :] + contract(tile_ref[:, here], values_ref[...])
        out_ref[here, :] = result + contract(basis_ref[:, here], dual)

    arguments = [which] + [in_vmem(value) for value in (total, tile, near)]
    arguments += [in_vmem(far[0])] + [in_hbm(piece) for piece in far[1:]]
    arguments += [in_vmem(value) for value in extra]
    in_specs = [pl.BlockSpec(memory_space=pltpu.SMEM)] + [whole() for _ in range(3)]
    in_specs += [whole()] + [pl.BlockSpec(memory_space=pltpu.HBM) for _ in far[1:]]
    in_specs += [whole() for _ in extra]
    return pl.pallas_call(
        kernel,
        grid=(points // block,),
        in_specs=in_specs,
        out_specs=whole(),
        out_shape=pltpu.VMEM((points, columns), jnp.float32),
        input_output_aliases={1: 0},
        compiler_params=grant(),
        scratch_shapes=[
            pltpu.VMEM((size, columns), jnp.bfloat16),
            pltpu.SemaphoreType.DMA((count,)),
        ],
        cost_estimate=pl.CostEstimate(
            flops=2 * size * points * columns,
            bytes_accessed=2 * size * columns,
            transcendentals=0,
        ),
    )(*arguments)


def add_last(total, flipped, far, near, which, column, out=None):
    points, columns = total.shape
    size, width = far.shape
    block = min(BLOCK // 2, points)
    steps = points // block
    here = pl.ds(column, width)

    def kernel(which_ref, total_ref, flipped_ref, far_ref, near_ref, *rest):
        out_ref, values_ref, staged_ref, sems = rest[-4:]

        def fetch():
            values_ref[...] = far_ref[...]

        choose(which_ref, fetch, near_ref.at[points - size :, here], values_ref)
        copies = []
        for step in range(steps):
            rows = pl.ds(step * block, block)
            staged_ref[rows, :] = total_ref[rows, here] + jnp.dot(
                flipped_ref[rows, :], values_ref[...], preferred_element_type=jnp.float32
            )
            copy = pltpu.make_async_copy(
                staged_ref.at[rows], out_ref.at[rows, here], sems.at[step]
            )
            copy.start()
            copies.append(copy)
        for copy in copies:
            copy.wait()

    arguments = [which] + [in_vmem(value) for value in (total, flipped, far, near)]
    in_specs = [pl.BlockSpec(memory_space=pltpu.SMEM)] + [whole() for _ in range(4)]
    if out is not None:
        arguments.append(in_hbm(out))
        in_specs.append(pl.BlockSpec(memory_space=pltpu.HBM))
    return pl.pallas_call(
        kernel,
        in_specs=in_specs,
        out_specs=pl.BlockSpec(memory_space=pltpu.HBM),
        out_shape=jax.ShapeDtypeStruct((points, columns), jnp.float32),
        input_output_aliases={} if out is None else {5: 0},
        compiler_params=grant(),
        scratch_shapes=[
            pltpu.VMEM((size, width), jnp.bfloat16),
            pltpu.VMEM((points, width), jnp.float32),
            pltpu.SemaphoreType.DMA((steps,)),
        ],
        cost_estimate=pl.CostEstimate(
            flops=2 * size * points * width,
            bytes_accessed=2 * size * points + 8 * points * width,
            transcendentals=0,
        ),
    )(*arguments)


def coupling_blocks(couplings, targets, ranks, count, rows, cols):
    slots, rank, _ = couplings.shape
    rank_index = jnp.arange(rank, dtype=jnp.int32)
    slot_index = jnp.arange(slots, dtype=jnp.int32)
    keep = (rank_index[None, :] < ranks[:, None]) & (slot_index < count)[:, None]
    keep = keep.astype(jnp.bfloat16)
    masked = couplings * keep[:, :, None] * keep[:, None, :]
    onehot = (targets[:, None] == jnp.arange(rows * cols, dtype=jnp.int32)[None, :]).astype(
        jnp.bfloat16
    )
    sums = contract(onehot, masked.reshape(slots, rank * rank))
    high = lax.reduce_precision(sums, 8, 7)
    parts = [high.astype(jnp.bfloat16), (sums - high).astype(jnp.bfloat16)]
    blocks = jnp.stack(parts).reshape(2, rows, cols, rank, rank).transpose(2, 3, 0, 1, 4)
    return blocks.reshape(cols, rank, 2 * rows * rank)


def dual_of(coefficients, blocks, rows, cols):
    rank, width = coefficients.shape
    packed = jnp.concatenate(
        [jnp.broadcast_to(coefficients[None], (cols,) + coefficients.shape), blocks], axis=2
    )
    me = lax.axis_index("col")
    held = [lax.dynamic_index_in_dim(packed, me, 0, keepdims=False)]
    for shift in range(1, cols):
        outgoing = lax.dynamic_index_in_dim(packed, (me + shift) % cols, 0, keepdims=False)
        held.append(lax.ppermute(outgoing, "col", [(i, (i + shift) % cols) for i in range(cols)]))
    held = jnp.concatenate(held, axis=0)
    half = width + rows * rank
    partial = contract(held[:, width:half], held[:, :width])
    partial = partial + contract(held[:, half:], held[:, :width])
    bits = rows.bit_length() - 1
    current = partial.reshape((2,) * bits + (rank, width))
    mine = lax.axis_index("row")
    left = list(range(bits))[::-1]
    order = [0] + list(range(bits - 1, 0, -1))
    for place, bit in enumerate(order):
        axis = left.index(bit)
        left.remove(bit)
        low = lax.index_in_dim(current, 0, axis, keepdims=False)
        high = lax.index_in_dim(current, 1, axis, keepdims=False)
        upper = (mine >> bit) & 1 == 1
        outgoing = jnp.where(upper, low, high)
        kept = jnp.where(upper, high, low)
        if place == bits - 1:
            outgoing = outgoing.astype(jnp.bfloat16)
        incoming = lax.ppermute(outgoing, "row", [(i, i ^ (1 << bit)) for i in range(rows)])
        if place < bits - 1:
            current = kept + incoming
    return kept, incoming


def on_device(
    residual,
    self_tiles,
    side_tiles,
    row_cluster_basis,
    column_cluster_basis,
    couplings,
    near_side,
    adm_targets,
    adm_ranks,
    adm_count,
):
    rows, cols = lax.axis_size("row"), lax.axis_size("col")
    local = residual[0, 0]
    points = local.shape[0]
    near_pairs = [(i, i ^ 1) for i in range(rows)]
    far_pairs = [(i, (i - 1) % rows if i % 2 == 0 else (i + 1) % rows) for i in range(rows)]
    side_offset = near_side[0, 0]
    near_offset = 1 - 2 * (lax.axis_index("row") % 2)
    which = jnp.where(
        side_offset == 0, 0, jnp.where(side_offset == near_offset, 1, 2)
    ).astype(jnp.int32).reshape(1)

    unit = points // 8
    lead = unit * 2
    width = local.shape[1]
    early = width * 3 // 4
    bounds = [
        (lead, 6 * unit - lead, 0, width),
        (6 * unit, 2 * unit, 0, early),
        (6 * unit, 2 * unit, early, width - early),
    ]
    pieces = list(split(local, [(0, lead, 0, width)]))
    *rest, coefficients = split(local, bounds, row_cluster_basis[0, 0].T)
    pieces += rest
    far = []
    for piece in pieces:
        far.append(lax.ppermute(piece, "row", far_pairs))
    near = lax.ppermute(local, "row", near_pairs)
    blocks = coupling_blocks(
        couplings[0, 0], adm_targets[0, 0], adm_ranks[0, 0], adm_count[0, 0], rows, cols
    )
    kept, incoming = dual_of(coefficients, blocks, rows, cols)
    total = own_product(self_tiles[0, 0], local, 0, 2)
    total = own_product(self_tiles[0, 0], local, 1, 2, total)
    side = side_tiles[0, 0]
    first, flipped, near, total = stage(side, near, total, 6 * unit)
    extra = (column_cluster_basis[0, 0].T, kept, incoming)
    total = add_rows(total, first, far[:2], near, which, extra)
    out = add_last(total, flipped, far[2], near, which, 0)
    out = add_last(total, flipped, far[3], near, which, early, out)
    return out[None, None]


def solution(mesh):
    placed = (
        P("row", "col", None, None),
        P("row", "col", None, None),
        P("row", "col", None, None),
        P("row", "col", None, None),
        P("row", "col", None, None),
        P("row", "col", None, None, None),
        P("row", "col"),
        P("row", "col", None),
        P("row", "col", None),
        P("row", "col"),
    )

    return jax.shard_map(
        on_device,
        mesh=mesh,
        in_specs=placed,
        out_specs=P("row", "col", None, None),
        check_vma=False,
    )
```

```python
import jax
import jax.numpy as jnp
from jax import lax
from jax.experimental import pallas as pl
from jax.experimental.pallas import tpu as pltpu
from jax.sharding import PartitionSpec as P

BLOCK = 512
GRANT = 20 * 1024 * 1024


def contract(tile, values):
    return lax.dot_general(
        tile, values, (((0,), (0,)), ((), ())), preferred_element_type=jnp.float32
    )


def in_vmem(value):
    return pltpu.with_memory_space_constraint(value, pltpu.VMEM)


def in_hbm(value):
    return pltpu.with_memory_space_constraint(value, pltpu.HBM)


def whole():
    return pl.BlockSpec(memory_space=pltpu.VMEM)


def grant():
    return pltpu.CompilerParams(vmem_limit_bytes=GRANT)


def split(values, bounds, basis=None):
    def kernel(values_ref, *rest):
        count, sems = len(bounds), rest[-1]
        outs = rest[:count] if basis is None else rest[1 : 1 + count]
        copies = [
            pltpu.make_async_copy(
                values_ref.at[pl.ds(row, size), pl.ds(column, width)], out, sems.at[c]
            )
            for c, ((row, size, column, width), out) in enumerate(zip(bounds, outs))
        ]
        if basis is not None:
            copies.append(pltpu.make_async_copy(values_ref, rest[-3], sems.at[count]))
            copies.append(pltpu.make_async_copy(rest[0], rest[-2], sems.at[count + 1]))
        for copy in copies:
            copy.start()
        for copy in copies:
            copy.wait()
        if basis is not None:
            sums_ref = rest[1 + count]
            sums_ref[...] = jnp.dot(
                rest[-2][...], rest[-3][...], preferred_element_type=jnp.float32
            ).astype(sums_ref.dtype)

    shapes = [(size, width) for _, size, _, width in bounds]
    arguments = [in_hbm(values)]
    scratch = []
    if basis is not None:
        arguments.append(in_hbm(basis))
        shapes.append((basis.shape[0], values.shape[1]))
        scratch = [pltpu.VMEM(value.shape, value.dtype) for value in (values, basis)]
    return pl.pallas_call(
        kernel,
        in_specs=[pl.BlockSpec(memory_space=pltpu.HBM) for _ in arguments],
        out_specs=[whole() for _ in shapes],
        out_shape=[pltpu.VMEM(shape, values.dtype) for shape in shapes],
        scratch_shapes=scratch + [pltpu.SemaphoreType.DMA((len(bounds) + 2,))],
        compiler_params=grant(),
    )(*arguments)


def own_product(tile, values, part, parts, total=None):
    points, columns = tile.shape[1], values.shape[1]
    block = min(BLOCK, points // parts)
    steps = points // parts // block
    first = part * steps

    def kernel(tile_ref, values_ref, *rest):
        rest[-1][...] = contract(tile_ref[...], values_ref[...])

    in_specs = [
        pl.BlockSpec((tile.shape[0], block), lambda i: (0, first + i)),
        pl.BlockSpec(values.shape, lambda i: (0, 0)),
    ]
    arguments = [in_hbm(tile), in_hbm(values)]
    if total is not None:
        in_specs.append(pl.BlockSpec(memory_space=pltpu.HBM))
        arguments.append(in_hbm(total))
    return pl.pallas_call(
        kernel,
        grid=(steps,),
        in_specs=in_specs,
        out_specs=pl.BlockSpec((block, columns), lambda i: (first + i, 0)),
        out_shape=pltpu.HBM((points, columns), jnp.float32),
        input_output_aliases={} if total is None else {2: 0},
        compiler_params=grant(),
        cost_estimate=pl.CostEstimate(
            flops=2 * tile.size * columns // parts,
            bytes_accessed=4 * tile.size // parts,
            transcendentals=0,
        ),
    )(*arguments)


def step_rows(block):
    return pl.ds(pl.multiple_of(pl.program_id(0) * block, block), block)


def stage(tile, near, total, which, start):
    rows, points = tile.shape
    size = rows - start
    block = min(BLOCK, points)

    def kernel(which_ref, tile_ref, near_ref, total_ref, first_ref, flipped_ref, *rest):
        near_out, total_out, last_ref, sems = rest
        near_copy = pltpu.make_async_copy(near_ref, near_out, sems.at[3])
        copies = [
            pltpu.make_async_copy(tile_ref.at[pl.ds(start, size)], last_ref, sems.at[0]),
            pltpu.make_async_copy(tile_ref.at[pl.ds(0, start)], first_ref, sems.at[1]),
            pltpu.make_async_copy(total_ref, total_out, sems.at[2]),
        ]
        for copy in copies:
            copy.start()

        @pl.when(which_ref[0] == 1)
        def _():
            near_copy.start()

        copies[0].wait()
        for at in range(0, points, block):
            flipped_ref[at : at + block, :] = last_ref[:, at : at + block].T
        for copy in copies[1:]:
            copy.wait()

        @pl.when(which_ref[0] == 1)
        def _():
            near_copy.wait()

    return pl.pallas_call(
        kernel,
        in_specs=[pl.BlockSpec(memory_space=pltpu.SMEM)]
        + [pl.BlockSpec(memory_space=pltpu.HBM) for _ in range(3)],
        out_specs=[whole() for _ in range(4)],
        out_shape=[
            pltpu.VMEM((start, points), tile.dtype),
            pltpu.VMEM((points, size), tile.dtype),
            pltpu.VMEM(near.shape, near.dtype),
            pltpu.VMEM(total.shape, total.dtype),
        ],
        compiler_params=grant(),
        scratch_shapes=[
            pltpu.VMEM((size, points), tile.dtype),
            pltpu.SemaphoreType.DMA((4,)),
        ],
    )(which, in_hbm(tile), in_hbm(near), in_hbm(total))


def add_rows(total, tile, flipped, far, near, which, extra):
    points, columns = total.shape
    size = tile.shape[0]
    block = min(BLOCK, points)
    count = len(far)
    steps = points // block

    def kernel(which_ref, total_ref, tile_ref, flipped_ref, near_ref, *rest):
        out_ref, final_ref, values_ref, sems, out_sems = rest[-5:]
        basis_ref, kept_ref, incoming_ref = rest[count:-5]
        here = step_rows(block)

        def fetch():
            lead = rest[0].shape[0]
            row, copies = lead, []
            values_ref[0:lead, :] = rest[0][...]
            for c, far_ref in enumerate(rest[1:count]):
                rows = pl.ds(row, far_ref.shape[0])
                copies.append(pltpu.make_async_copy(far_ref, values_ref.at[rows], sems.at[c]))
                copies[-1].start()
                row += far_ref.shape[0]
            for copy in copies:
                copy.wait()

        @pl.when((pl.program_id(0) == 0) & (which_ref[0] == 2))
        def _():
            fetch()

        dual = (kept_ref[...] + incoming_ref[...].astype(jnp.float32)).astype(jnp.bfloat16)
        out_ref[here, :] = total_ref[here, :] + contract(basis_ref[:, here], dual)

        @pl.when(which_ref[0] == 2)
        def _():
            out_ref[here, :] += contract(tile_ref[:, here], values_ref[...])

        @pl.when(which_ref[0] == 1)
        def _():
            result = contract(tile_ref[:, here], near_ref[:size, :])
            out_ref[here, :] += result + jnp.dot(
                flipped_ref[here, :], near_ref[size:, :], preferred_element_type=jnp.float32
            )

        def finished(step):
            rows = pl.ds(step * block, block)
            return pltpu.make_async_copy(
                out_ref.at[rows], final_ref.at[rows], out_sems.at[step]
            )

        @pl.when(which_ref[0] != 2)
        def _():
            pltpu.make_async_copy(
                out_ref.at[here], final_ref.at[here], out_sems.at[pl.program_id(0)]
            ).start()

        @pl.when((which_ref[0] != 2) & (pl.program_id(0) == steps - 1))
        def _():
            for step in range(steps):
                finished(step).wait()

    arguments = [which] + [in_vmem(value) for value in (total, tile, flipped, near)]
    arguments += [in_vmem(far[0])] + [in_hbm(piece) for piece in far[1:]]
    arguments += [in_vmem(value) for value in extra]
    in_specs = [pl.BlockSpec(memory_space=pltpu.SMEM)] + [whole() for _ in range(4)]
    in_specs += [whole()] + [pl.BlockSpec(memory_space=pltpu.HBM) for _ in far[1:]]
    in_specs += [whole() for _ in extra]
    return pl.pallas_call(
        kernel,
        grid=(steps,),
        in_specs=in_specs,
        out_specs=[whole(), pl.BlockSpec(memory_space=pltpu.HBM)],
        out_shape=[
            pltpu.VMEM((points, columns), jnp.float32),
            pltpu.HBM((points, columns), jnp.float32),
        ],
        input_output_aliases={1: 0},
        compiler_params=grant(),
        scratch_shapes=[
            pltpu.VMEM((size, columns), jnp.bfloat16),
            pltpu.SemaphoreType.DMA((count,)),
            pltpu.SemaphoreType.DMA((steps,)),
        ],
        cost_estimate=pl.CostEstimate(
            flops=2 * size * points * columns,
            bytes_accessed=2 * size * columns,
            transcendentals=0,
        ),
    )(*arguments)


def add_last(total, flipped, far, which, column, out):
    points, columns = total.shape
    size, width = far.shape
    block = min(BLOCK // 2, points)
    steps = points // block
    here = pl.ds(column, width)

    def kernel(which_ref, total_ref, flipped_ref, far_ref, *rest):
        out_ref, staged_ref, sems = rest[-3:]

        @pl.when(which_ref[0] == 2)
        def _():
            copies = []
            for step in range(steps):
                rows = pl.ds(step * block, block)
                staged_ref[rows, :] = total_ref[rows, here] + jnp.dot(
                    flipped_ref[rows, :], far_ref[...], preferred_element_type=jnp.float32
                )
                copy = pltpu.make_async_copy(
                    staged_ref.at[rows], out_ref.at[rows, here], sems.at[step]
                )
                copy.start()
                copies.append(copy)
            for copy in copies:
                copy.wait()

    arguments = [which] + [in_vmem(value) for value in (total, flipped, far)]
    in_specs = [pl.BlockSpec(memory_space=pltpu.SMEM)] + [whole() for _ in range(3)]
    arguments.append(in_hbm(out))
    in_specs.append(pl.BlockSpec(memory_space=pltpu.HBM))
    return pl.pallas_call(
        kernel,
        in_specs=in_specs,
        out_specs=pl.BlockSpec(memory_space=pltpu.HBM),
        out_shape=jax.ShapeDtypeStruct((points, columns), jnp.float32),
        input_output_aliases={4: 0},
        compiler_params=grant(),
        scratch_shapes=[
            pltpu.VMEM((points, width), jnp.float32),
            pltpu.SemaphoreType.DMA((steps,)),
        ],
        cost_estimate=pl.CostEstimate(
            flops=2 * size * points * width,
            bytes_accessed=2 * size * points + 8 * points * width,
            transcendentals=0,
        ),
    )(*arguments)


def coupling_blocks(couplings, targets, ranks, count, rows, cols):
    slots, rank, _ = couplings.shape
    rank_index = jnp.arange(rank, dtype=jnp.int32)
    slot_index = jnp.arange(slots, dtype=jnp.int32)
    keep = (rank_index[None, :] < ranks[:, None]) & (slot_index < count)[:, None]
    keep = keep.astype(jnp.bfloat16)
    masked = couplings * keep[:, :, None] * keep[:, None, :]
    onehot = (targets[:, None] == jnp.arange(rows * cols, dtype=jnp.int32)[None, :]).astype(
        jnp.bfloat16
    )
    sums = contract(onehot, masked.reshape(slots, rank * rank))
    high = lax.reduce_precision(sums, 8, 7)
    parts = [high.astype(jnp.bfloat16), (sums - high).astype(jnp.bfloat16)]
    blocks = jnp.stack(parts).reshape(2, rows, cols, rank, rank).transpose(2, 3, 0, 1, 4)
    return blocks.reshape(cols, rank, 2 * rows * rank)


def dual_of(coefficients, blocks, rows, cols):
    rank, width = coefficients.shape
    packed = jnp.concatenate(
        [jnp.broadcast_to(coefficients[None], (cols,) + coefficients.shape), blocks], axis=2
    )
    me = lax.axis_index("col")
    held = [lax.dynamic_index_in_dim(packed, me, 0, keepdims=False)]
    for shift in range(1, cols):
        outgoing = lax.dynamic_index_in_dim(packed, (me + shift) % cols, 0, keepdims=False)
        held.append(lax.ppermute(outgoing, "col", [(i, (i + shift) % cols) for i in range(cols)]))
    held = jnp.concatenate(held, axis=0)
    half = width + rows * rank
    partial = contract(held[:, width:half], held[:, :width])
    partial = partial + contract(held[:, half:], held[:, :width])
    bits = rows.bit_length() - 1
    current = partial.reshape((2,) * bits + (rank, width))
    mine = lax.axis_index("row")
    left = list(range(bits))[::-1]
    order = [0] + list(range(bits - 1, 0, -1))
    for place, bit in enumerate(order):
        axis = left.index(bit)
        left.remove(bit)
        low = lax.index_in_dim(current, 0, axis, keepdims=False)
        high = lax.index_in_dim(current, 1, axis, keepdims=False)
        upper = (mine >> bit) & 1 == 1
        outgoing = jnp.where(upper, low, high)
        kept = jnp.where(upper, high, low)
        if place == bits - 1:
            outgoing = outgoing.astype(jnp.bfloat16)
        incoming = lax.ppermute(outgoing, "row", [(i, i ^ (1 << bit)) for i in range(rows)])
        if place < bits - 1:
            current = kept + incoming
    return kept, incoming


def on_device(
    residual,
    self_tiles,
    side_tiles,
    row_cluster_basis,
    column_cluster_basis,
    couplings,
    near_side,
    adm_targets,
    adm_ranks,
    adm_count,
):
    rows, cols = lax.axis_size("row"), lax.axis_size("col")
    local = residual[0, 0]
    points = local.shape[0]
    near_pairs = [(i, i ^ 1) for i in range(rows)]
    far_pairs = [(i, (i - 1) % rows if i % 2 == 0 else (i + 1) % rows) for i in range(rows)]
    side_offset = near_side[0, 0]
    near_offset = 1 - 2 * (lax.axis_index("row") % 2)
    which = jnp.where(
        side_offset == 0, 0, jnp.where(side_offset == near_offset, 1, 2)
    ).astype(jnp.int32).reshape(1)

    unit = points // 8
    lead = unit * 2
    width = local.shape[1]
    early = width * 3 // 4
    bounds = [
        (lead, 6 * unit - lead, 0, width),
        (6 * unit, 2 * unit, 0, early),
        (6 * unit, 2 * unit, early, width - early),
    ]
    pieces = list(split(local, [(0, lead, 0, width)]))
    *rest, coefficients = split(local, bounds, row_cluster_basis[0, 0].T)
    pieces += rest
    far = []
    for piece in pieces:
        far.append(lax.ppermute(piece, "row", far_pairs))
    near = lax.ppermute(local, "row", near_pairs)
    blocks = coupling_blocks(
        couplings[0, 0], adm_targets[0, 0], adm_ranks[0, 0], adm_count[0, 0], rows, cols
    )
    kept, incoming = dual_of(coefficients, blocks, rows, cols)
    total = own_product(self_tiles[0, 0], local, 0, 2)
    total = own_product(self_tiles[0, 0], local, 1, 2, total)
    side = side_tiles[0, 0]
    first, flipped, near, total = stage(side, near, total, which, 6 * unit)
    extra = (column_cluster_basis[0, 0].T, kept, incoming)
    total, out = add_rows(total, first, flipped, far[:2], near, which, extra)
    out = add_last(total, flipped, far[2], which, 0, out)
    out = add_last(total, flipped, far[3], which, early, out)
    return out[None, None]


def solution(mesh):
    placed = (
        P("row", "col", None, None),
        P("row", "col", None, None),
        P("row", "col", None, None),
        P("row", "col", None, None),
        P("row", "col", None, None),
        P("row", "col", None, None, None),
        P("row", "col"),
        P("row", "col", None),
        P("row", "col", None),
        P("row", "col"),
    )

    return jax.shard_map(
        on_device,
        mesh=mesh,
        in_specs=placed,
        out_specs=P("row", "col", None, None),
        check_vma=False,
    )
```

```python
import jax
import jax.numpy as jnp
from jax import lax
from jax.experimental import pallas as pl
from jax.experimental.pallas import tpu as pltpu
from jax.sharding import PartitionSpec as P

BLOCK = 512
GRANT = 20 * 1024 * 1024


def contract(tile, values):
    return lax.dot_general(
        tile, values, (((0,), (0,)), ((), ())), preferred_element_type=jnp.float32
    )


def in_vmem(value):
    return pltpu.with_memory_space_constraint(value, pltpu.VMEM)


def in_hbm(value):
    return pltpu.with_memory_space_constraint(value, pltpu.HBM)


def whole():
    return pl.BlockSpec(memory_space=pltpu.VMEM)


def grant():
    return pltpu.CompilerParams(vmem_limit_bytes=GRANT)


def split(values, bounds, basis=None):
    def kernel(values_ref, *rest):
        count, sems = len(bounds), rest[-1]
        outs = rest[:count] if basis is None else rest[1 : 1 + count]
        copies = [
            pltpu.make_async_copy(
                values_ref.at[pl.ds(row, size), pl.ds(column, width)], out, sems.at[c]
            )
            for c, ((row, size, column, width), out) in enumerate(zip(bounds, outs))
        ]
        if basis is not None:
            copies.append(pltpu.make_async_copy(values_ref, rest[-3], sems.at[count]))
            copies.append(pltpu.make_async_copy(rest[0], rest[-2], sems.at[count + 1]))
        for copy in copies:
            copy.start()
        for copy in copies:
            copy.wait()
        if basis is not None:
            sums_ref = rest[1 + count]
            sums_ref[...] = jnp.dot(
                rest[-2][...], rest[-3][...], preferred_element_type=jnp.float32
            ).astype(sums_ref.dtype)

    shapes = [(size, width) for _, size, _, width in bounds]
    arguments = [in_hbm(values)]
    scratch = []
    if basis is not None:
        arguments.append(in_hbm(basis))
        shapes.append((basis.shape[0], values.shape[1]))
        scratch = [pltpu.VMEM(value.shape, value.dtype) for value in (values, basis)]
    return pl.pallas_call(
        kernel,
        in_specs=[pl.BlockSpec(memory_space=pltpu.HBM) for _ in arguments],
        out_specs=[whole() for _ in shapes],
        out_shape=[pltpu.VMEM(shape, values.dtype) for shape in shapes],
        scratch_shapes=scratch + [pltpu.SemaphoreType.DMA((len(bounds) + 2,))],
        compiler_params=grant(),
    )(*arguments)


def own_product(tile, values, part, parts, total=None):
    points, columns = tile.shape[1], values.shape[1]
    block = min(BLOCK, points // parts)
    steps = points // parts // block
    first = part * steps

    def kernel(tile_ref, values_ref, *rest):
        rest[-1][...] = contract(tile_ref[...], values_ref[...])

    in_specs = [
        pl.BlockSpec((tile.shape[0], block), lambda i: (0, first + i)),
        pl.BlockSpec(values.shape, lambda i: (0, 0)),
    ]
    arguments = [in_hbm(tile), in_hbm(values)]
    if total is not None:
        in_specs.append(pl.BlockSpec(memory_space=pltpu.HBM))
        arguments.append(in_hbm(total))
    return pl.pallas_call(
        kernel,
        grid=(steps,),
        in_specs=in_specs,
        out_specs=pl.BlockSpec((block, columns), lambda i: (first + i, 0)),
        out_shape=pltpu.HBM((points, columns), jnp.float32),
        input_output_aliases={} if total is None else {2: 0},
        compiler_params=grant(),
        cost_estimate=pl.CostEstimate(
            flops=2 * tile.size * columns // parts,
            bytes_accessed=4 * tile.size // parts,
            transcendentals=0,
        ),
    )(*arguments)


def step_rows(block):
    return pl.ds(pl.multiple_of(pl.program_id(0) * block, block), block)


def stage(tile, near, total, which, start):
    rows, points = tile.shape
    size = rows - start
    block = min(BLOCK, points)

    def kernel(which_ref, tile_ref, near_ref, total_ref, first_ref, flipped_ref, *rest):
        near_out, total_out, last_ref, sems = rest
        near_copy = pltpu.make_async_copy(near_ref, near_out, sems.at[3])
        copies = [
            pltpu.make_async_copy(tile_ref.at[pl.ds(start, size)], last_ref, sems.at[0]),
            pltpu.make_async_copy(tile_ref.at[pl.ds(0, start)], first_ref, sems.at[1]),
            pltpu.make_async_copy(total_ref, total_out, sems.at[2]),
        ]
        for copy in copies:
            copy.start()

        @pl.when(which_ref[0] == 1)
        def _():
            near_copy.start()

        copies[0].wait()
        for at in range(0, points, block):
            flipped_ref[at : at + block, :] = last_ref[:, at : at + block].T
        for copy in copies[1:]:
            copy.wait()

        @pl.when(which_ref[0] == 1)
        def _():
            near_copy.wait()

    return pl.pallas_call(
        kernel,
        in_specs=[pl.BlockSpec(memory_space=pltpu.SMEM)]
        + [pl.BlockSpec(memory_space=pltpu.HBM) for _ in range(3)],
        out_specs=[whole() for _ in range(4)],
        out_shape=[
            pltpu.VMEM((start, points), tile.dtype),
            pltpu.VMEM((points, size), tile.dtype),
            pltpu.VMEM(near.shape, near.dtype),
            pltpu.VMEM(total.shape, total.dtype),
        ],
        compiler_params=grant(),
        scratch_shapes=[
            pltpu.VMEM((size, points), tile.dtype),
            pltpu.SemaphoreType.DMA((4,)),
        ],
    )(which, in_hbm(tile), in_hbm(near), in_hbm(total))


def add_rows(total, tile, flipped, far, near, which, extra):
    points, columns = total.shape
    size = tile.shape[0]
    block = min(BLOCK, points)
    count = len(far)
    steps = points // block

    def kernel(which_ref, total_ref, tile_ref, flipped_ref, near_ref, *rest):
        out_ref, final_ref, values_ref, sems, out_sems = rest[-5:]
        basis_ref, kept_ref, incoming_ref = rest[count:-5]
        here = step_rows(block)

        def fetch():
            lead = rest[0].shape[0]
            row, copies = lead, []
            values_ref[0:lead, :] = rest[0][...]
            for c, far_ref in enumerate(rest[1:count]):
                rows = pl.ds(row, far_ref.shape[0])
                copies.append(pltpu.make_async_copy(far_ref, values_ref.at[rows], sems.at[c]))
                copies[-1].start()
                row += far_ref.shape[0]
            for copy in copies:
                copy.wait()

        @pl.when((pl.program_id(0) == 0) & (which_ref[0] == 2))
        def _():
            fetch()

        dual = (kept_ref[...] + incoming_ref[...].astype(jnp.float32)).astype(jnp.bfloat16)

        def base():
            return total_ref[here, :] + contract(basis_ref[:, here], dual)

        @pl.when(which_ref[0] == 2)
        def _():
            out_ref[here, :] = base() + contract(tile_ref[:, here], values_ref[...])

        @pl.when(which_ref[0] == 1)
        def _():
            result = base() + contract(tile_ref[:, here], near_ref[:size, :])
            out_ref[here, :] = result + jnp.dot(
                flipped_ref[here, :], near_ref[size:, :], preferred_element_type=jnp.float32
            )

        @pl.when(which_ref[0] == 0)
        def _():
            out_ref[here, :] = base()

        def finished(step):
            rows = pl.ds(step * block, block)
            return pltpu.make_async_copy(
                out_ref.at[rows], final_ref.at[rows], out_sems.at[step]
            )

        @pl.when(which_ref[0] != 2)
        def _():
            pltpu.make_async_copy(
                out_ref.at[here], final_ref.at[here], out_sems.at[pl.program_id(0)]
            ).start()

        @pl.when((which_ref[0] != 2) & (pl.program_id(0) == steps - 1))
        def _():
            for step in range(steps):
                finished(step).wait()

    arguments = [which] + [in_vmem(value) for value in (total, tile, flipped, near)]
    arguments += [in_vmem(far[0])] + [in_hbm(piece) for piece in far[1:]]
    arguments += [in_vmem(value) for value in extra]
    in_specs = [pl.BlockSpec(memory_space=pltpu.SMEM)] + [whole() for _ in range(4)]
    in_specs += [whole()] + [pl.BlockSpec(memory_space=pltpu.HBM) for _ in far[1:]]
    in_specs += [whole() for _ in extra]
    return pl.pallas_call(
        kernel,
        grid=(steps,),
        in_specs=in_specs,
        out_specs=[whole(), pl.BlockSpec(memory_space=pltpu.HBM)],
        out_shape=[
            pltpu.VMEM((points, columns), jnp.float32),
            pltpu.HBM((points, columns), jnp.float32),
        ],
        input_output_aliases={1: 0},
        compiler_params=grant(),
        scratch_shapes=[
            pltpu.VMEM((size, columns), jnp.bfloat16),
            pltpu.SemaphoreType.DMA((count,)),
            pltpu.SemaphoreType.DMA((steps,)),
        ],
        cost_estimate=pl.CostEstimate(
            flops=2 * size * points * columns,
            bytes_accessed=2 * size * columns,
            transcendentals=0,
        ),
    )(*arguments)


def add_last(total, flipped, far, which, column, out):
    points, columns = total.shape
    size, width = far.shape
    block = min(BLOCK // 2, points)
    steps = points // block
    here = pl.ds(column, width)

    def kernel(which_ref, total_ref, flipped_ref, far_ref, *rest):
        out_ref, staged_ref, sems = rest[-3:]

        @pl.when(which_ref[0] == 2)
        def _():
            copies = []
            for step in range(steps):
                rows = pl.ds(step * block, block)
                staged_ref[rows, :] = total_ref[rows, here] + jnp.dot(
                    flipped_ref[rows, :], far_ref[...], preferred_element_type=jnp.float32
                )
                copy = pltpu.make_async_copy(
                    staged_ref.at[rows], out_ref.at[rows, here], sems.at[step]
                )
                copy.start()
                copies.append(copy)
            for copy in copies:
                copy.wait()

    arguments = [which] + [in_vmem(value) for value in (total, flipped, far)]
    in_specs = [pl.BlockSpec(memory_space=pltpu.SMEM)] + [whole() for _ in range(3)]
    arguments.append(in_hbm(out))
    in_specs.append(pl.BlockSpec(memory_space=pltpu.HBM))
    return pl.pallas_call(
        kernel,
        in_specs=in_specs,
        out_specs=pl.BlockSpec(memory_space=pltpu.HBM),
        out_shape=jax.ShapeDtypeStruct((points, columns), jnp.float32),
        input_output_aliases={4: 0},
        compiler_params=grant(),
        scratch_shapes=[
            pltpu.VMEM((points, width), jnp.float32),
            pltpu.SemaphoreType.DMA((steps,)),
        ],
        cost_estimate=pl.CostEstimate(
            flops=2 * size * points * width,
            bytes_accessed=2 * size * points + 8 * points * width,
            transcendentals=0,
        ),
    )(*arguments)


def coupling_blocks(couplings, targets, ranks, count, rows, cols):
    slots, rank, _ = couplings.shape
    rank_index = jnp.arange(rank, dtype=jnp.int32)
    slot_index = jnp.arange(slots, dtype=jnp.int32)
    keep = (rank_index[None, :] < ranks[:, None]) & (slot_index < count)[:, None]
    keep = keep.astype(jnp.bfloat16)
    masked = couplings * keep[:, :, None] * keep[:, None, :]
    onehot = (targets[:, None] == jnp.arange(rows * cols, dtype=jnp.int32)[None, :]).astype(
        jnp.bfloat16
    )
    sums = contract(onehot, masked.reshape(slots, rank * rank))
    high = lax.reduce_precision(sums, 8, 7)
    parts = [high.astype(jnp.bfloat16), (sums - high).astype(jnp.bfloat16)]
    blocks = jnp.stack(parts).reshape(2, rows, cols, rank, rank).transpose(2, 3, 0, 1, 4)
    return blocks.reshape(cols, rank, 2 * rows * rank)


def dual_of(coefficients, blocks, rows, cols):
    rank, width = coefficients.shape
    packed = jnp.concatenate(
        [jnp.broadcast_to(coefficients[None], (cols,) + coefficients.shape), blocks], axis=2
    )
    me = lax.axis_index("col")
    held = [lax.dynamic_index_in_dim(packed, me, 0, keepdims=False)]
    for shift in range(1, cols):
        outgoing = lax.dynamic_index_in_dim(packed, (me + shift) % cols, 0, keepdims=False)
        held.append(lax.ppermute(outgoing, "col", [(i, (i + shift) % cols) for i in range(cols)]))
    held = jnp.concatenate(held, axis=0)
    half = width + rows * rank
    partial = contract(held[:, width:half], held[:, :width])
    partial = partial + contract(held[:, half:], held[:, :width])
    bits = rows.bit_length() - 1
    current = partial.reshape((2,) * bits + (rank, width))
    mine = lax.axis_index("row")
    left = list(range(bits))[::-1]
    order = [0] + list(range(bits - 1, 0, -1))
    for place, bit in enumerate(order):
        axis = left.index(bit)
        left.remove(bit)
        low = lax.index_in_dim(current, 0, axis, keepdims=False)
        high = lax.index_in_dim(current, 1, axis, keepdims=False)
        upper = (mine >> bit) & 1 == 1
        outgoing = jnp.where(upper, low, high)
        kept = jnp.where(upper, high, low)
        if place == bits - 1:
            outgoing = outgoing.astype(jnp.bfloat16)
        incoming = lax.ppermute(outgoing, "row", [(i, i ^ (1 << bit)) for i in range(rows)])
        if place < bits - 1:
            current = kept + incoming
    return kept, incoming


def on_device(
    residual,
    self_tiles,
    side_tiles,
    row_cluster_basis,
    column_cluster_basis,
    couplings,
    near_side,
    adm_targets,
    adm_ranks,
    adm_count,
):
    rows, cols = lax.axis_size("row"), lax.axis_size("col")
    local = residual[0, 0]
    points = local.shape[0]
    near_pairs = [(i, i ^ 1) for i in range(rows)]
    far_pairs = [(i, (i - 1) % rows if i % 2 == 0 else (i + 1) % rows) for i in range(rows)]
    side_offset = near_side[0, 0]
    near_offset = 1 - 2 * (lax.axis_index("row") % 2)
    which = jnp.where(
        side_offset == 0, 0, jnp.where(side_offset == near_offset, 1, 2)
    ).astype(jnp.int32).reshape(1)

    unit = points // 8
    lead = unit * 2
    width = local.shape[1]
    early = width * 3 // 4
    bounds = [
        (lead, 6 * unit - lead, 0, width),
        (6 * unit, 2 * unit, 0, early),
        (6 * unit, 2 * unit, early, width - early),
    ]
    pieces = list(split(local, [(0, lead, 0, width)]))
    *rest, coefficients = split(local, bounds, row_cluster_basis[0, 0].T)
    pieces += rest
    far = []
    for piece in pieces:
        far.append(lax.ppermute(piece, "row", far_pairs))
    near = lax.ppermute(local, "row", near_pairs)
    blocks = coupling_blocks(
        couplings[0, 0], adm_targets[0, 0], adm_ranks[0, 0], adm_count[0, 0], rows, cols
    )
    kept, incoming = dual_of(coefficients, blocks, rows, cols)
    total = own_product(self_tiles[0, 0], local, 0, 2)
    total = own_product(self_tiles[0, 0], local, 1, 2, total)
    side = side_tiles[0, 0]
    first, flipped, near, total = stage(side, near, total, which, 6 * unit)
    extra = (column_cluster_basis[0, 0].T, kept, incoming)
    total, out = add_rows(total, first, flipped, far[:2], near, which, extra)
    out = add_last(total, flipped, far[2], which, 0, out)
    out = add_last(total, flipped, far[3], which, early, out)
    return out[None, None]


def solution(mesh):
    placed = (
        P("row", "col", None, None),
        P("row", "col", None, None),
        P("row", "col", None, None),
        P("row", "col", None, None),
        P("row", "col", None, None),
        P("row", "col", None, None, None),
        P("row", "col"),
        P("row", "col", None),
        P("row", "col", None),
        P("row", "col"),
    )

    return jax.shard_map(
        on_device,
        mesh=mesh,
        in_specs=placed,
        out_specs=P("row", "col", None, None),
        check_vma=False,
    )
```
